32 devices in a mesh: dp: 4 (over x, core), mp: 8 (over z, y).
Axes of the slice: x: 2, y: 2, z: 4, core: 2. Of those that a mesh axis runs over, the one named last changes fastest.
Arguments:
- sensitivity: bfloat16 [4096, 16, 1024], P('dp', 'mp'), may hold values from -0.046875 to 0.046875
- observed: float32 [4096], P('dp'), may hold values from -6 to 6
- row_weight: float32 [4096], P('dp'), may hold values from 1 to 8
- model: float32 [2, 16, 1024], P(None, 'mp'), may hold values from -3 to 3
- smooth_weight: float32 [16, 1024], P('mp'), may hold values from 0.5 to 2
- active: int32 [2, 16, 1024], P(None, 'mp'), may hold values 0 or 1
Outputs:
- update: float32 [2, 16, 1024], P(None, 'mp')
- cg_residual: float32 [2, 16, 1024], P(None, 'mp')
The draws below stay inside these ranges and needn't reach their ends.
All inputs are finite; a program needn't handle non-finite values. No bound on the sum of `active` on one device may be relied on, other than what follows from the above.
Results may differ from the reference program's by a relative error of at most 0.018.
Values sent between devices are 32-bit elements; how exact they have to be, the bound alone decides.
No kernel may reach another device: no remote copies, remote signals or barrier semaphores. Data moves between devices by JAX's collectives and lax.ppermute only.
A program may use at most 64 MiB of HBM per device.

```python
import math
import jax
import jax.numpy as jnp

GY = 64
GZ = 16
ITERS = 4
GX = 16
ROWS = 4096


def touch_ends(values, stream_key, low, top_value):
    longest = values.shape.index(max(values.shape))
    spots = []
    for shift in (0, 1):
        where = [jax.random.randint(jax.random.fold_in(stream_key, axis), (), 0, length) for axis, length in enumerate(values.shape)]
        where[longest] = (where[longest] + shift) % values.shape[longest]
        spots.append(tuple(where))
    return values.at[spots[0]].set(low).at[spots[1]].set(top_value)


def shard_levels(rng, dims, shards, low, high):
    def one(dim, blocks):
        draws = jax.random.uniform(jax.random.fold_in(jax.random.fold_in(rng, 6), dim), (blocks,), jnp.float32, low / len(shards), high / len(shards))
        return jnp.repeat(jnp.exp(draws), dims[dim] // blocks).reshape((-1,) + (1,) * (len(dims) - dim - 1))

    loudness = one(*shards[0])
    for cut in shards[1:]:
        loudness = loudness * one(*cut)
    return loudness


def noise(own_key, shape, spread, limit, cuts=(), held_as=jnp.bfloat16):
    values = spread * jax.random.normal(own_key, shape, jnp.float32)
    if cuts:
        values = values * shard_levels(own_key, shape, cuts, -0.22, 0.18)
    return jnp.clip(values, -limit, limit).astype(held_as)


def setup_inputs(seed: int = 0) -> dict:
    streams_of = jax.random.split(jax.random.key(seed), 7)
    return {
        "sensitivity": noise(streams_of[0], (ROWS, GX, GY * GZ), (GX * GY * GZ) ** -0.5, 0.046875, ((0, 4), (1, 8))),
        "observed": noise(streams_of[1], (ROWS,), 1.0, 6.0, ((0, 4),), jnp.float32),
        "row_weight": jnp.clip(jnp.exp(math.log(8.0) - 2.0794415 * jax.random.uniform(streams_of[2], (ROWS,), jnp.float32) ** shard_levels(streams_of[2], (ROWS,), ((0, 4),), -0.2, 0.2)), 1.0, 8.0),
        "model": noise(streams_of[3], (2, GX, GY * GZ), 0.5, 3.0, ((1, 8),), jnp.float32),
        "smooth_weight": jnp.clip(jnp.exp(math.log(2.0) - 1.3862944 * jax.random.uniform(streams_of[4], (GX, GY * GZ), jnp.float32) ** shard_levels(streams_of[4], (GX, GY * GZ), ((0, 8),), -0.2, 0.2)), 0.5, 2.0),
        "active": touch_ends((jax.random.randint(streams_of[5], (2, GX, GY * GZ), 0, 4) < 1).astype(jnp.int32), jax.random.fold_in(streams_of[5], 1), 0, 1),
    }


SMOOTHING = 0.25
COUPLING = 0.5


def inner_sum(field, column_len):
    width = field.shape[-1]
    position = jnp.arange(width) % column_len
    blank_one = jnp.zeros_like(field[..., :1])
    blank_col = jnp.zeros_like(field[..., :column_len])
    later = jnp.where(position != column_len - 1, jnp.concatenate([field[..., 1:], blank_one], -1), 0.0)
    earlier = jnp.where(position != 0, jnp.concatenate([blank_one, field[..., :-1]], -1), 0.0)
    ahead = jnp.concatenate([field[..., column_len:], blank_col], -1)
    behind = jnp.concatenate([blank_col, field[..., :-column_len]], -1)
    return later + earlier + ahead + behind


def operate(field, smooth_weight):
    padded = jnp.pad(field, ((0, 0), (1, 1), (0, 0)))
    beside = padded[:, 2:] + padded[:, :-2] + inner_sum(field, GZ)
    return smooth_weight * field + SMOOTHING * (6.0 * field - beside) + COUPLING * (field - field[::-1])


def reference(sensitivity, observed, row_weight, model, smooth_weight, active):
    rows = sensitivity.shape[0]
    split = rows * 3 // 4
    matrix = sensitivity.reshape(rows, -1)
    upper = matrix[:split]
    lower = matrix[split:]
    free_mask = 1.0 - active.astype(jnp.float32)
    cell_shape = model.shape

    def forward(field):
        flattened = field.reshape(2, -1).astype(jnp.bfloat16)
        return jnp.concatenate([jnp.dot(upper, flattened[0], preferred_element_type=jnp.float32),
                                jnp.dot(lower, flattened[1], preferred_element_type=jnp.float32)])

    def adjoint(values, regular):
        scaled = (row_weight * values).astype(jnp.bfloat16)
        summed = jnp.stack([jnp.dot(scaled[:split], upper, preferred_element_type=jnp.float32),
                            jnp.dot(scaled[split:], lower, preferred_element_type=jnp.float32)])
        return free_mask * (summed.reshape(cell_shape) + regular)

    residual = -adjoint(forward(model) - observed, operate(model, smooth_weight))
    direction = residual
    solution = jnp.zeros_like(model)
    norm_now = jnp.sum(residual * residual)
    for step in range(ITERS):
        image = adjoint(forward(direction), operate(direction, smooth_weight))
        step_len = norm_now / jnp.sum(direction * image)
        solution = solution + step_len * direction
        residual = residual - step_len * image
        norm_next = jnp.sum(residual * residual)
        direction = residual + (norm_next / norm_now) * direction
        norm_now = norm_next
    return solution, residual
```

```python
import jax
import jax.numpy as jnp
from jax import lax
from jax.sharding import PartitionSpec as P

GZ = 16
ITERS = 4


SMOOTHING = 0.25
COUPLING = 0.5
LANES = 128


def inner_sum(field, column_len):
    width = field.shape[-1]
    position = jnp.arange(width) % column_len
    blank_one = jnp.zeros_like(field[..., :1])
    blank_col = jnp.zeros_like(field[..., :column_len])
    later = jnp.where(
        position != column_len - 1, jnp.concatenate([field[..., 1:], blank_one], -1), 0.0
    )
    earlier = jnp.where(position != 0, jnp.concatenate([blank_one, field[..., :-1]], -1), 0.0)
    ahead = jnp.concatenate([field[..., column_len:], blank_col], -1)
    behind = jnp.concatenate([blank_col, field[..., :-column_len]], -1)
    return later + earlier + ahead + behind


def operate_inner(field, smooth_weight):
    padded = jnp.pad(field, ((0, 0), (1, 1), (0, 0)))
    beside = padded[:, 2:] + padded[:, :-2] + inner_sum(field, GZ)
    return (
        smooth_weight * field
        + SMOOTHING * (6.0 * field - beside)
        + COUPLING * (field - field[::-1])
    )


def tree_sum(parts):
    while len(parts) > 1:
        parts = [parts[i] + parts[i + 1] for i in range(0, len(parts), 2)]
    return parts[0]


def local(sensitivity, observed, row_weight, model, smooth_weight, active):
    rows = sensitivity.shape[0]
    matrix = sensitivity.reshape(rows, -1)
    cells = matrix.shape[1]
    width = model.shape[2]
    rank = lax.axis_index("mp")
    owners = lax.axis_size("mp")
    block = lax.axis_index("dp")
    blocks = lax.axis_size("dp")
    split = blocks * 3 // 4
    gravity_rows = block < split
    free_mask = 1.0 - active.astype(jnp.float32)

    def exchange_rows(field, scalars):
        flattened = field.reshape(2, -1)
        chosen = jnp.where(gravity_rows, flattened[0], flattened[1]).astype(jnp.bfloat16)
        partial_rows = jnp.dot(matrix, chosen, preferred_element_type=jnp.float32)
        tail = jnp.stack(scalars) if scalars else jnp.zeros((0,), jnp.float32)
        message = jnp.concatenate(
            [
                partial_rows,
                field[:, 0].reshape(-1),
                field[:, -1].reshape(-1),
                tail,
                jnp.zeros((LANES - tail.shape[0],), jnp.float32),
            ]
        )
        sent = jnp.broadcast_to(message, (owners,) + message.shape)
        got = lax.all_to_all(sent, "mp", 0, 0, tiled=True)
        total = got[:, :rows].sum(0)
        first = got[:, rows : rows + 2 * width].reshape(owners, 2, width)
        last = got[:, rows + 2 * width : rows + 4 * width].reshape(owners, 2, width)
        sums = got[:, rows + 4 * width :].sum(0)
        below = jnp.where(rank > 0, lax.dynamic_index_in_dim(last, jnp.maximum(rank - 1, 0), 0, False), 0.0)
        above = jnp.where(
            rank < owners - 1,
            lax.dynamic_index_in_dim(first, jnp.minimum(rank + 1, owners - 1), 0, False),
            0.0,
        )
        cross = -2.0 * SMOOTHING * jnp.sum(last[:-1] * first[1:])
        return total, below, above, cross, sums

    def exchange_cells(values):
        scaled = (row_weight * values).astype(jnp.bfloat16)
        columns = jnp.dot(scaled, matrix, preferred_element_type=jnp.float32)
        weighed = jnp.sum(values * scaled.astype(jnp.float32))
        message = jnp.concatenate([columns, jnp.broadcast_to(weighed, (LANES,))])
        parts = [message] + [
            lax.ppermute(message, "dp", [(i, i ^ s) for i in range(blocks)])
            for s in range(1, blocks)
        ]
        gravity = [(block ^ s) < split for s in range(blocks)]
        density = tree_sum([jnp.where(g, p[:cells], 0.0) for g, p in zip(gravity, parts)])
        susceptibility = tree_sum([jnp.where(g, 0.0, p[:cells]) for g, p in zip(gravity, parts)])
        summed = jnp.stack([density, susceptibility]).reshape(model.shape)
        return summed, tree_sum([p[cells] for p in parts])

    def finish(inner, below, above):
        inner = inner.at[:, 0].add(-SMOOTHING * below)
        return inner.at[:, -1].add(-SMOOTHING * above)

    inner = operate_inner(model, smooth_weight)
    predicted, below, above, _, _ = exchange_rows(model, [])
    summed, _ = exchange_cells(predicted - observed)
    residual = -free_mask * (summed + finish(inner, below, above))

    direction = jnp.zeros_like(residual)
    imaged = jnp.zeros_like(residual)
    solution = jnp.zeros_like(residual)
    norm_before = None
    curvature = None
    for step in range(ITERS):
        inner = operate_inner(residual, smooth_weight)
        scalars = [
            jnp.sum(residual * residual),
            jnp.sum(residual * inner),
            jnp.sum(residual * imaged),
        ]
        projected, below, above, cross, sums = exchange_rows(residual, scalars)
        summed, weighed = exchange_cells(projected)
        image = free_mask * (summed + finish(inner, below, above))
        norm_now = sums[0]
        own = weighed + sums[1] + cross
        if step:
            ratio = norm_now / norm_before
            curvature = own + ratio * (2.0 * sums[2] + ratio * curvature)
            direction = residual + ratio * direction
            imaged = image + ratio * imaged
        else:
            curvature = own
            direction = residual
            imaged = image
        step_len = norm_now / curvature
        solution = solution + step_len * direction
        residual = residual - step_len * imaged
        norm_before = norm_now
    return (solution, residual)


def solution(mesh):
    return jax.shard_map(
        local,
        mesh=mesh,
        in_specs=(
            P("dp", "mp", None),
            P("dp"),
            P("dp"),
            P(None, "mp", None),
            P("mp", None),
            P(None, "mp", None),
        ),
        out_specs=(P(None, "mp", None), P(None, "mp", None)),
        check_vma=False,
    )
```

```python
import functools

import jax
import jax.numpy as jnp
from jax import lax
from jax.experimental import pallas as pl
from jax.experimental.pallas import tpu as pltpu
from jax.sharding import PartitionSpec as P

GZ = 16
ITERS = 4


SMOOTHING = 0.25
COUPLING = 0.5
LANES = 128
SUBLANES = 8
KERNEL_VMEM = 16 * 1024 * 1024


def tree_sum(parts):
    while len(parts) > 1:
        parts = [parts[i] + parts[i + 1] for i in range(0, len(parts), 2)]
    return parts[0]


def inner_sum(plane):
    tall = plane.shape[0]
    lane = lax.broadcasted_iota(jnp.int32, plane.shape, 1)
    line = lax.broadcasted_iota(jnp.int32, plane.shape, 0)
    position = lane % GZ
    later = jnp.where(position != GZ - 1, pltpu.roll(plane, LANES - 1, 1), 0.0)
    earlier = jnp.where(position != 0, pltpu.roll(plane, 1, 1), 0.0)
    ahead = pltpu.roll(plane, LANES - GZ, 1)
    over = jnp.where(line < tall - 1, pltpu.roll(ahead, tall - 1, 0), 0.0)
    ahead = jnp.where(lane < LANES - GZ, ahead, over)
    behind = pltpu.roll(plane, GZ, 1)
    under = jnp.where(line > 0, pltpu.roll(behind, 1, 0), 0.0)
    behind = jnp.where(lane >= GZ, behind, under)
    return later + earlier + ahead + behind


def operate_inner(field, smooth_weight):
    layers = len(field[0])
    out = [[], []]
    for f in range(2):
        for i in range(layers):
            own = field[f][i]
            beside = inner_sum(own)
            if i:
                beside = beside + field[f][i - 1]
            if i < layers - 1:
                beside = beside + field[f][i + 1]
            out[f].append(
                smooth_weight[i] * own
                + SMOOTHING * (6.0 * own - beside)
                + COUPLING * (own - field[1 - f][i])
            )
    return out


def load(ref):
    return [[ref[f, i] for i in range(ref.shape[1])] for f in range(2)]


def store(ref, field):
    for f in range(2):
        for i in range(ref.shape[1]):
            ref[f, i] = field[f][i]


def mapped(op, *fields):
    return [[op(*(x[f][i] for x in fields)) for i in range(len(fields[0][0]))] for f in range(2)]


def dot_line(one, two):
    total = None
    for f in range(2):
        for i in range(len(one[0])):
            term = one[f][i] * two[f][i]
            total = term if total is None else total + term
    return jnp.sum(total, axis=0, keepdims=True)


def full(line):
    return jnp.sum(line, axis=1, keepdims=True)


def spread(planes, count):
    return jnp.concatenate(
        [
            jnp.broadcast_to(plane[t : t + 1], (count, LANES))
            for plane in planes
            for t in range(plane.shape[0])
        ],
        axis=1,
    )


def send_rows(place_ref, matrix_ref, field, lines, out_ref):
    owners = out_ref.shape[0]
    rows = matrix_ref.shape[0]
    tall = field[0][0].shape[0]
    gravity_rows = place_ref[1] < place_ref[2]
    chosen = [jnp.where(gravity_rows, d, s) for d, s in zip(field[0], field[1])]
    vector = spread(chosen, LANES).astype(jnp.bfloat16)
    eye = lax.broadcasted_iota(jnp.int32, (LANES, LANES), 0) == lax.broadcasted_iota(
        jnp.int32, (LANES, LANES), 1
    )
    product = lax.dot_general(
        matrix_ref[...], vector, (((1,), (1,)), ((), ())), preferred_element_type=jnp.float32
    )
    pieces = [
        jnp.sum(
            jnp.where(eye, product[b * LANES : (b + 1) * LANES], 0.0), axis=0, keepdims=True
        )
        for b in range(rows // LANES)
    ]
    pieces += [field[0][0], field[1][0], field[0][-1], field[1][-1]]
    pieces += lines
    pieces.append(jnp.zeros((SUBLANES - len(lines), LANES), jnp.float32))
    message = jnp.concatenate(pieces, axis=0)
    for j in range(owners):
        out_ref[j] = message


def start_kernel(place_ref, matrix_ref, model_ref, out_ref):
    send_rows(place_ref, matrix_ref, load(model_ref), [], out_ref)


def rows_kernel(matrix_ref, got_ref, weight_ref, observed_ref, out_ref, *, subtract):
    owners = got_ref.shape[0]
    rows, cells = matrix_ref.shape
    blocks = rows // LANES
    values = got_ref[0, 0:blocks]
    for j in range(1, owners):
        values = values + got_ref[j, 0:blocks]
    if subtract:
        values = values - observed_ref[...]
    scaled = (weight_ref[...] * values).astype(jnp.bfloat16).astype(jnp.float32)
    weighed = jnp.sum(values * scaled, axis=0, keepdims=True)
    vector = spread([scaled], 2 * SUBLANES).astype(jnp.bfloat16)
    columns = jnp.dot(vector, matrix_ref[...], preferred_element_type=jnp.float32)
    pieces = [columns[0:1, t * LANES : (t + 1) * LANES] for t in range(cells // LANES)]
    pieces += [weighed, jnp.zeros((SUBLANES - 1, LANES), jnp.float32)]
    out_ref[...] = jnp.concatenate(pieces, axis=0)


def gathered(place_ref, part_refs, got_ref, inner_ref, mask_ref, base):
    rank = place_ref[0]
    owners = got_ref.shape[0]
    layers, tall = inner_ref.shape[1:3]
    cells = layers * tall
    gravity = [(place_ref[1] ^ s) < place_ref[2] for s in range(len(part_refs))]
    parts = [ref[0:cells] for ref in part_refs]
    data = [
        tree_sum([jnp.where(g, p, 0.0) for g, p in zip(gravity, parts)]),
        tree_sum([jnp.where(g, 0.0, p) for g, p in zip(gravity, parts)]),
    ]
    down = jnp.maximum(rank - 1, 0)
    up = jnp.minimum(rank + 1, owners - 1)
    image = [[], []]
    for f in range(2):
        first = base + f * tall
        last = base + (2 + f) * tall
        below = jnp.where(rank > 0, got_ref[down, last : last + tall], 0.0)
        above = jnp.where(rank < owners - 1, got_ref[up, first : first + tall], 0.0)
        for i in range(layers):
            regular = inner_ref[f, i]
            if i == 0:
                regular = regular - SMOOTHING * below
            if i == layers - 1:
                regular = regular - SMOOTHING * above
            image[f].append(mask_ref[f, i] * (data[f][i * tall : (i + 1) * tall] + regular))
    return image


def first_kernel(place_ref, matrix_ref, *refs, count, base):
    part_refs = refs[:count]
    got_ref, model_ref, smooth_ref, mask_ref, out_ref, residual_ref, inner_ref, held = refs[count:]
    layers = model_ref.shape[1]
    smooth_weight = [smooth_ref[i] for i in range(layers)]
    store(held, operate_inner(load(model_ref), smooth_weight))
    image = gathered(place_ref, part_refs, got_ref, held, mask_ref, base)
    residual = mapped(lambda a: -a, image)
    inner = operate_inner(residual, smooth_weight)
    store(residual_ref, residual)
    store(inner_ref, inner)
    lines = [dot_line(residual, residual), dot_line(residual, inner)]
    send_rows(place_ref, matrix_ref, residual, lines, out_ref)


def cells_kernel(place_ref, matrix_ref, *refs, count, base, begin, final):
    part_refs = refs[:count]
    got_ref, smooth_ref, mask_ref, residual_in, inner_in = refs[count : count + 5]
    refs = refs[count + 5 :]
    if not begin:
        direction_in, imaged_in, solution_in, norms_in = refs[:4]
        refs = refs[4:]
    solution_ref, residual_ref = refs[:2]
    owners = got_ref.shape[0]
    layers, tall = inner_in.shape[1:3]
    cells = layers * tall
    residual = load(residual_in)
    image = gathered(place_ref, part_refs, got_ref, inner_in, mask_ref, base)
    at = base + 4 * tall
    sums = got_ref[0, at : at + SUBLANES]
    for j in range(1, owners):
        sums = sums + got_ref[j, at : at + SUBLANES]
    cross = None
    for j in range(owners - 1):
        term = (
            got_ref[j, base + 2 * tall : base + 4 * tall] * got_ref[j + 1, base : base + 2 * tall]
        )
        cross = term if cross is None else cross + term
    weighed = tree_sum([ref[cells : cells + 1] for ref in part_refs])
    line = weighed + sums[1:2]
    line = line - 2.0 * SMOOTHING * jnp.sum(cross, axis=0, keepdims=True)
    norm_now = full(sums[0:1])
    curvature = full(line)
    if begin:
        direction, imaged = residual, image
    else:
        ratio = norm_now / norms_in[0:1, 0:1]
        curvature = curvature + ratio * (2.0 * full(sums[2:3]) + ratio * norms_in[1:2, 0:1])
        direction = mapped(lambda r, d: r + ratio * d, residual, load(direction_in))
        imaged = mapped(lambda r, d: r + ratio * d, image, load(imaged_in))
    step_len = norm_now / curvature
    if begin:
        update = mapped(lambda d: step_len * d, direction)
    else:
        update = mapped(lambda x, d: x + step_len * d, load(solution_in), direction)
    residual = mapped(lambda r, s: r - step_len * s, residual, imaged)
    store(solution_ref, update)
    store(residual_ref, residual)
    if final:
        return
    direction_ref, imaged_ref, norms_ref, inner_ref, out_ref = refs[2:]
    store(direction_ref, direction)
    store(imaged_ref, imaged)
    norms_ref[0:1] = jnp.broadcast_to(norm_now, (1, LANES))
    norms_ref[1:2] = jnp.broadcast_to(curvature, (1, LANES))
    inner = operate_inner(residual, [smooth_ref[i] for i in range(layers)])
    store(inner_ref, inner)
    lines = [dot_line(residual, residual), dot_line(residual, inner), dot_line(residual, imaged)]
    send_rows(place_ref, matrix_ref, residual, lines, out_ref)


def local(sensitivity, observed, row_weight, model, smooth_weight, active):
    rows = sensitivity.shape[0]
    matrix = sensitivity.reshape(rows, -1)
    layers, width = smooth_weight.shape
    tall = width // LANES
    owners = lax.axis_size("mp")
    blocks = lax.axis_size("dp")
    place = jnp.stack(
        [lax.axis_index("mp"), lax.axis_index("dp"), jnp.int32(blocks * 3 // 4)]
    ).astype(jnp.int32)
    base = rows // LANES

    def planes(x):
        return x.reshape(x.shape[:-1] + (tall, LANES))

    mask = planes(1.0 - active.astype(jnp.float32))
    smooth = planes(smooth_weight)
    weight = row_weight.reshape(base, LANES)
    target = observed.reshape(base, LANES)
    start = planes(model)
    matrix = pltpu.with_memory_space_constraint(matrix, pltpu.VMEM)

    cell = jax.ShapeDtypeStruct(start.shape, jnp.float32)
    message = jax.ShapeDtypeStruct(
        (owners, base + 4 * tall + SUBLANES, LANES), jnp.float32
    )
    columns = jax.ShapeDtypeStruct((layers * tall + SUBLANES, LANES), jnp.float32)
    norms = jax.ShapeDtypeStruct((2, LANES), jnp.float32)
    smem = pl.BlockSpec(memory_space=pltpu.SMEM)
    vmem = pl.BlockSpec(memory_space=pltpu.VMEM)

    def call(kernel, out_shape, *operands, name, scratch=(), scalars=True):
        specs = [smem] * scalars + [vmem] * len(operands)
        operands = ((place,) if scalars else ()) + operands
        return pl.pallas_call(
            kernel,
            out_shape=out_shape,
            in_specs=specs,
            out_specs=jax.tree.map(lambda _: vmem, out_shape),
            scratch_shapes=scratch,
            compiler_params=pltpu.CompilerParams(vmem_limit_bytes=KERNEL_VMEM),
            name=name,
        )(*operands)

    def across(sent):
        return lax.all_to_all(sent, "mp", 0, 0, tiled=True)

    def along(got, subtract):
        sent = call(
            functools.partial(rows_kernel, subtract=subtract),
            columns,
            matrix,
            got,
            weight,
            target,
            name="rows",
            scalars=False,
        )
        return [sent] + [
            lax.ppermute(sent, "dp", [(i, i ^ s) for i in range(blocks)])
            for s in range(1, blocks)
        ]

    got = across(call(start_kernel, message, matrix, start, name="start"))
    parts = along(got, True)
    sent, residual, inner = call(
        functools.partial(first_kernel, count=blocks, base=base),
        (message, cell, cell),
        matrix,
        *parts,
        got,
        start,
        smooth,
        mask,
        name="first",
        scratch=[pltpu.VMEM(start.shape, jnp.float32)],
    )
    carried = ()
    for step in range(ITERS):
        got = across(sent)
        parts = along(got, False)
        final = step == ITERS - 1
        outs = (cell, cell) if final else (cell, cell, cell, cell, norms, cell, message)
        result = call(
            functools.partial(
                cells_kernel, count=blocks, base=base, begin=step == 0, final=final
            ),
            outs,
            matrix,
            *parts,
            got,
            smooth,
            mask,
            residual,
            inner,
            *carried,
            name="cells",
        )
        if final:
            update, residual = result
        else:
            update, residual, direction, imaged, scalars, inner, sent = result
            carried = (direction, imaged, update, scalars)
    return (update.reshape(model.shape), residual.reshape(model.shape))


def solution(mesh):
    return jax.shard_map(
        local,
        mesh=mesh,
        in_specs=(
            P("dp", "mp", None),
            P("dp"),
            P("dp"),
            P(None, "mp", None),
            P("mp", None),
            P(None, "mp", None),
        ),
        out_specs=(P(None, "mp", None), P(None, "mp", None)),
        check_vma=False,
    )
```

```python
import functools

import jax
import jax.numpy as jnp
from jax import lax
from jax.experimental import pallas as pl
from jax.experimental.pallas import tpu as pltpu
from jax.sharding import PartitionSpec as P

GZ = 16
ITERS = 4


SMOOTHING = 0.25
COUPLING = 0.5
LANES = 128
SUBLANES = 8
KERNEL_VMEM = 16 * 1024 * 1024


def tree_sum(parts):
    while len(parts) > 1:
        parts = [parts[i] + parts[i + 1] for i in range(0, len(parts), 2)]
    return parts[0]


def inner_sum(plane):
    tall = plane.shape[0]
    lane = lax.broadcasted_iota(jnp.int32, plane.shape, 1)
    line = lax.broadcasted_iota(jnp.int32, plane.shape, 0)
    position = lane % GZ
    later = jnp.where(position != GZ - 1, pltpu.roll(plane, LANES - 1, 1), 0.0)
    earlier = jnp.where(position != 0, pltpu.roll(plane, 1, 1), 0.0)
    ahead = pltpu.roll(plane, LANES - GZ, 1)
    over = jnp.where(line < tall - 1, pltpu.roll(ahead, tall - 1, 0), 0.0)
    ahead = jnp.where(lane < LANES - GZ, ahead, over)
    behind = pltpu.roll(plane, GZ, 1)
    under = jnp.where(line > 0, pltpu.roll(behind, 1, 0), 0.0)
    behind = jnp.where(lane >= GZ, behind, under)
    return later + earlier + ahead + behind


def operate_inner(field, smooth_weight):
    layers = len(field[0])
    out = [[], []]
    for f in range(2):
        for i in range(layers):
            own = field[f][i]
            beside = inner_sum(own)
            if i:
                beside = beside + field[f][i - 1]
            if i < layers - 1:
                beside = beside + field[f][i + 1]
            out[f].append(
                smooth_weight[i] * own
                + SMOOTHING * (6.0 * own - beside)
                + COUPLING * (own - field[1 - f][i])
            )
    return out


def load(ref):
    return [[ref[f, i] for i in range(ref.shape[1])] for f in range(2)]


def store(ref, field):
    for f in range(2):
        for i in range(ref.shape[1]):
            ref[f, i] = field[f][i]


def mapped(op, *fields):
    return [[op(*(x[f][i] for x in fields)) for i in range(len(fields[0][0]))] for f in range(2)]


def dot_line(one, two):
    total = None
    for f in range(2):
        for i in range(len(one[0])):
            term = one[f][i] * two[f][i]
            total = term if total is None else total + term
    return jnp.sum(total, axis=0, keepdims=True)


def full(line):
    return jnp.sum(line, axis=1, keepdims=True)


def spread(planes, count):
    return jnp.concatenate(
        [
            jnp.broadcast_to(plane[t : t + 1], (count, LANES))
            for plane in planes
            for t in range(plane.shape[0])
        ],
        axis=1,
    )


def rows_between(plane, low, count):
    line = lax.broadcasted_iota(jnp.int32, plane.shape, 0)
    return (line >= low) & (line < low + count)


def share_of(planes, member, members):
    tall = planes[0].shape[0]
    count = tall // members
    out = jnp.zeros_like(planes[0])
    for n, plane in enumerate(planes):
        moved = pltpu.roll(plane, (n * count - member * count + tall) % tall, 0)
        out = jnp.where(rows_between(plane, n * count, count), moved, out)
    return out


def from_shares(shares, members, n):
    tall = shares[0][1].shape[0]
    count = tall // members
    out = jnp.zeros_like(shares[0][1])
    for member, share in shares:
        moved = pltpu.roll(share, (member * count - n * count + tall) % tall, 0)
        out = jnp.where(rows_between(share, member * count, count), moved, out)
    return out


def send_rows(place_ref, matrix_ref, field, lines, out_ref, members):
    owners = out_ref.shape[0]
    rows = matrix_ref.shape[0]
    tall = field[0][0].shape[0]
    gravity_rows = place_ref[1] < place_ref[2]
    chosen = [jnp.where(gravity_rows, d, s) for d, s in zip(field[0], field[1])]
    vector = spread(chosen, LANES).astype(jnp.bfloat16)
    eye = lax.broadcasted_iota(jnp.int32, (LANES, LANES), 0) == lax.broadcasted_iota(
        jnp.int32, (LANES, LANES), 1
    )
    product = lax.dot_general(
        matrix_ref[...], vector, (((1,), (1,)), ((), ())), preferred_element_type=jnp.float32
    )
    pieces = [
        jnp.sum(
            jnp.where(eye, product[b * LANES : (b + 1) * LANES], 0.0), axis=0, keepdims=True
        )
        for b in range(rows // LANES)
    ]
    edges = [field[0][0], field[1][0], field[0][-1], field[1][-1]]
    pieces.append(share_of(edges, place_ref[1], members))
    pieces += lines
    pieces.append(jnp.zeros((SUBLANES - len(lines), LANES), jnp.float32))
    message = jnp.concatenate(pieces, axis=0)
    for j in range(owners):
        out_ref[j] = message


def load_layers(ref):
    layers, width = ref.shape
    return [
        jnp.concatenate([ref[i : i + 1, t : t + LANES] for t in range(0, width, LANES)], axis=0)
        for i in range(layers)
    ]


def load_wide(ref):
    return [load_layers(ref.at[f]) for f in range(2)]


def store_wide(ref, field):
    for f in range(2):
        for i in range(ref.shape[1]):
            for t in range(ref.shape[2] // LANES):
                ref[f, i : i + 1, t * LANES : (t + 1) * LANES] = field[f][i][t : t + 1]


def start_kernel(place_ref, matrix_ref, model_ref, out_ref, *, members):
    send_rows(place_ref, matrix_ref, load_wide(model_ref), [], out_ref, members)


def rows_kernel(
    place_ref, matrix_ref, got_ref, weight_ref, observed_ref, out_ref, *, subtract, members, tall
):
    rank = place_ref[0]
    owners = got_ref.shape[0]
    rows, cells = matrix_ref.shape
    blocks = rows // LANES
    values = got_ref[0, 0:blocks]
    for j in range(1, owners):
        values = values + got_ref[j, 0:blocks]
    if subtract:
        values = values - observed_ref[...]
    scaled = (weight_ref[...] * values).astype(jnp.bfloat16).astype(jnp.float32)
    weighed = jnp.sum(values * scaled, axis=0, keepdims=True)
    vector = spread([scaled], 2 * SUBLANES).astype(jnp.bfloat16)
    columns = jnp.dot(vector, matrix_ref[...], preferred_element_type=jnp.float32)
    pieces = [columns[0:1, t * LANES : (t + 1) * LANES] for t in range(cells // LANES)]
    half = 2 * (tall // members)
    shares = [got_ref[j, blocks : blocks + tall] for j in range(owners)]
    lower = rows_between(shares[0], 0, half)
    upper = rows_between(shares[0], half, half)
    cross = None
    for j in range(owners - 1):
        term = shares[j] * pltpu.roll(shares[j + 1], half, 0)
        cross = term if cross is None else cross + term
    cross = jnp.sum(jnp.where(upper, cross, 0.0), axis=0, keepdims=True)
    weighed = weighed - 2.0 * SMOOTHING * cross
    down = jnp.maximum(rank - 1, 0)
    up = jnp.minimum(rank + 1, owners - 1)
    above = jnp.where(lower & (rank < owners - 1), got_ref[up, blocks : blocks + tall], 0.0)
    below = jnp.where(upper & (rank > 0), got_ref[down, blocks : blocks + tall], 0.0)
    pieces += [above + below, weighed, jnp.zeros((SUBLANES - 1, LANES), jnp.float32)]
    out_ref[...] = jnp.concatenate(pieces, axis=0)


def gathered(place_ref, part_refs, inner_ref, mask_ref):
    layers, tall = inner_ref.shape[1:3]
    cells = layers * tall
    members = len(part_refs)
    sources = [place_ref[1] ^ s for s in range(members)]
    gravity = [q < place_ref[2] for q in sources]
    parts = [ref[0:cells] for ref in part_refs]
    data = [
        tree_sum([jnp.where(g, p, 0.0) for g, p in zip(gravity, parts)]),
        tree_sum([jnp.where(g, 0.0, p) for g, p in zip(gravity, parts)]),
    ]
    shares = [(q, ref[cells : cells + tall]) for q, ref in zip(sources, part_refs)]
    image = [[], []]
    for f in range(2):
        above = from_shares(shares, members, f)
        below = from_shares(shares, members, 2 + f)
        for i in range(layers):
            regular = inner_ref[f, i]
            if i == 0:
                regular = regular - SMOOTHING * below
            if i == layers - 1:
                regular = regular - SMOOTHING * above
            image[f].append(mask_ref[f, i] * (data[f][i * tall : (i + 1) * tall] + regular))
    return image


def first_kernel(place_ref, matrix_ref, *refs, count):
    part_refs = refs[:count]
    model_ref, weight_ref, active_ref, out_ref, residual_ref, inner_ref = refs[count : count + 6]
    smooth_ref, mask_ref, held = refs[count + 6 :]
    layers = model_ref.shape[1]
    smooth_weight = load_layers(weight_ref)
    for i in range(layers):
        smooth_ref[i] = smooth_weight[i]
    store(mask_ref, mapped(lambda a: 1.0 - a.astype(jnp.float32), load_wide(active_ref)))
    store(held, operate_inner(load_wide(model_ref), smooth_weight))
    image = gathered(place_ref, part_refs, held, mask_ref)
    residual = mapped(lambda a: -a, image)
    inner = operate_inner(residual, smooth_weight)
    store(residual_ref, residual)
    store(inner_ref, inner)
    lines = [dot_line(residual, residual), dot_line(residual, inner)]
    send_rows(place_ref, matrix_ref, residual, lines, out_ref, count)


def cells_kernel(place_ref, matrix_ref, *refs, count, base, begin, final):
    part_refs = refs[:count]
    got_ref, smooth_ref, mask_ref, residual_in, inner_in = refs[count : count + 5]
    refs = refs[count + 5 :]
    if not begin:
        direction_in, imaged_in, solution_in, norms_in = refs[:4]
        refs = refs[4:]
    solution_ref, residual_ref = refs[:2]
    owners = got_ref.shape[0]
    layers, tall = inner_in.shape[1:3]
    cells = layers * tall
    residual = load(residual_in)
    image = gathered(place_ref, part_refs, inner_in, mask_ref)
    at = base + tall
    sums = got_ref[0, at : at + SUBLANES]
    for j in range(1, owners):
        sums = sums + got_ref[j, at : at + SUBLANES]
    at = cells + tall
    weighed = tree_sum([ref[at : at + 1] for ref in part_refs])
    line = weighed + sums[1:2]
    norm_now = full(sums[0:1])
    curvature = full(line)
    if begin:
        direction, imaged = residual, image
    else:
        ratio = norm_now / norms_in[0:1, 0:1]
        curvature = curvature + ratio * (2.0 * full(sums[2:3]) + ratio * norms_in[1:2, 0:1])
        direction = mapped(lambda r, d: r + ratio * d, residual, load(direction_in))
        imaged = mapped(lambda r, d: r + ratio * d, image, load(imaged_in))
    step_len = norm_now / curvature
    if begin:
        update = mapped(lambda d: step_len * d, direction)
    else:
        update = mapped(lambda x, d: x + step_len * d, load(solution_in), direction)
    residual = mapped(lambda r, s: r - step_len * s, residual, imaged)
    if final:
        store_wide(solution_ref, update)
        store_wide(residual_ref, residual)
        return
    store(solution_ref, update)
    store(residual_ref, residual)
    direction_ref, imaged_ref, norms_ref, inner_ref, out_ref = refs[2:]
    store(direction_ref, direction)
    store(imaged_ref, imaged)
    norms_ref[0:1] = jnp.broadcast_to(norm_now, (1, LANES))
    norms_ref[1:2] = jnp.broadcast_to(curvature, (1, LANES))
    inner = operate_inner(residual, [smooth_ref[i] for i in range(layers)])
    store(inner_ref, inner)
    lines = [dot_line(residual, residual), dot_line(residual, inner), dot_line(residual, imaged)]
    send_rows(place_ref, matrix_ref, residual, lines, out_ref, count)


def local(sensitivity, observed, row_weight, model, smooth_weight, active):
    rows = sensitivity.shape[0]
    matrix = sensitivity.reshape(rows, -1)
    layers, width = smooth_weight.shape
    tall = width // LANES
    owners = lax.axis_size("mp")
    blocks = lax.axis_size("dp")
    place = jnp.stack(
        [lax.axis_index("mp"), lax.axis_index("dp"), jnp.int32(blocks * 3 // 4)]
    ).astype(jnp.int32)
    base = rows // LANES

    weight = row_weight.reshape(base, LANES)
    target = observed.reshape(base, LANES)

    cell = jax.ShapeDtypeStruct((2, layers, tall, LANES), jnp.float32)
    field = jax.ShapeDtypeStruct(cell.shape[1:], jnp.float32)
    wide = jax.ShapeDtypeStruct(model.shape, jnp.float32)
    if tall % blocks or blocks < 4:
        raise ValueError("boundary shares")
    message = jax.ShapeDtypeStruct((owners, base + tall + SUBLANES, LANES), jnp.float32)
    columns = jax.ShapeDtypeStruct(((layers + 1) * tall + SUBLANES, LANES), jnp.float32)
    norms = jax.ShapeDtypeStruct((2, LANES), jnp.float32)
    smem = pl.BlockSpec(memory_space=pltpu.SMEM)
    vmem = pl.BlockSpec(memory_space=pltpu.VMEM)

    def call(kernel, out_shape, *operands, name, scratch=()):
        held = pltpu.with_memory_space_constraint(matrix, pltpu.VMEM)
        return pl.pallas_call(
            kernel,
            out_shape=out_shape,
            in_specs=[smem] + [vmem] * (1 + len(operands)),
            out_specs=jax.tree.map(lambda _: vmem, out_shape),
            scratch_shapes=scratch,
            compiler_params=pltpu.CompilerParams(vmem_limit_bytes=KERNEL_VMEM),
            name=name,
        )(place, held, *operands)

    def across(sent):
        return lax.all_to_all(sent, "mp", 0, 0, tiled=True)

    def along(got, subtract):
        sent = call(
            functools.partial(rows_kernel, subtract=subtract, members=blocks, tall=tall),
            columns,
            got,
            weight,
            target,
            name="rows",
        )
        return [sent] + [
            lax.ppermute(sent, "dp", [(i, i ^ s) for i in range(blocks)])
            for s in range(1, blocks)
        ]

    got = across(call(functools.partial(start_kernel, members=blocks), message, model, name="start"))
    parts = along(got, True)
    sent, residual, inner, smooth, mask = call(
        functools.partial(first_kernel, count=blocks),
        (message, cell, cell, field, cell),
        *parts,
        model,
        smooth_weight,
        active,
        name="first",
        scratch=[pltpu.VMEM(cell.shape, jnp.float32)],
    )
    carried = ()
    for step in range(ITERS):
        got = across(sent)
        parts = along(got, False)
        final = step == ITERS - 1
        outs = (wide, wide) if final else (cell, cell, cell, cell, norms, cell, message)
        result = call(
            functools.partial(
                cells_kernel, count=blocks, base=base, begin=step == 0, final=final
            ),
            outs,
            *parts,
            got,
            smooth,
            mask,
            residual,
            inner,
            *carried,
            name="cells",
        )
        if final:
            update, residual = result
        else:
            update, residual, direction, imaged, scalars, inner, sent = result
            carried = (direction, imaged, update, scalars)
    return (update, residual)


def solution(mesh):
    return jax.shard_map(
        local,
        mesh=mesh,
        in_specs=(
            P("dp", "mp", None),
            P("dp"),
            P("dp"),
            P(None, "mp", None),
            P("mp", None),
            P(None, "mp", None),
        ),
        out_specs=(P(None, "mp", None), P(None, "mp", None)),
        check_vma=False,
    )
```

```python
import functools

import jax
import jax.numpy as jnp
from jax import lax
from jax.experimental import pallas as pl
from jax.experimental.pallas import tpu as pltpu
from jax.sharding import PartitionSpec as P

GZ = 16
ITERS = 4


SMOOTHING = 0.25
COUPLING = 0.5
LANES = 128
SUBLANES = 8
KERNEL_VMEM = 16 * 1024 * 1024


def tree_sum(parts):
    while len(parts) > 1:
        parts = [parts[i] + parts[i + 1] for i in range(0, len(parts), 2)]
    return parts[0]


def inner_sum(plane):
    tall = plane.shape[0]
    lane = lax.broadcasted_iota(jnp.int32, plane.shape, 1)
    line = lax.broadcasted_iota(jnp.int32, plane.shape, 0)
    position = lane % GZ
    later = jnp.where(position != GZ - 1, pltpu.roll(plane, LANES - 1, 1), 0.0)
    earlier = jnp.where(position != 0, pltpu.roll(plane, 1, 1), 0.0)
    ahead = pltpu.roll(plane, LANES - GZ, 1)
    over = jnp.where(line < tall - 1, pltpu.roll(ahead, tall - 1, 0), 0.0)
    ahead = jnp.where(lane < LANES - GZ, ahead, over)
    behind = pltpu.roll(plane, GZ, 1)
    under = jnp.where(line > 0, pltpu.roll(behind, 1, 0), 0.0)
    behind = jnp.where(lane >= GZ, behind, under)
    return later + earlier + ahead + behind


def operate_inner(field, smooth_weight):
    layers = len(field[0])
    out = [[], []]
    for f in range(2):
        for i in range(layers):
            own = field[f][i]
            beside = inner_sum(own)
            if i:
                beside = beside + field[f][i - 1]
            if i < layers - 1:
                beside = beside + field[f][i + 1]
            out[f].append(
                smooth_weight[i] * own
                + SMOOTHING * (6.0 * own - beside)
                + COUPLING * (own - field[1 - f][i])
            )
    return out


def load(ref):
    return [[ref[f, i] for i in range(ref.shape[1])] for f in range(2)]


def store(ref, field):
    for f in range(2):
        for i in range(ref.shape[1]):
            ref[f, i] = field[f][i]


def mapped(op, *fields):
    return [[op(*(x[f][i] for x in fields)) for i in range(len(fields[0][0]))] for f in range(2)]


def dot_line(one, two):
    total = None
    for f in range(2):
        for i in range(len(one[0])):
            term = one[f][i] * two[f][i]
            total = term if total is None else total + term
    return jnp.sum(total, axis=0, keepdims=True)


def full(line):
    return jnp.sum(line, axis=1, keepdims=True)


def spread(planes, count):
    return jnp.concatenate(
        [
            jnp.broadcast_to(plane[t : t + 1], (count, LANES))
            for plane in planes
            for t in range(plane.shape[0])
        ],
        axis=1,
    )


def where_block(shape, count, block, members):
    line = lax.broadcasted_iota(jnp.int32, shape, 0)
    return line // count == lax.rem(block, jnp.int32(members))


def share_of(planes, member, members):
    tall = planes[0].shape[0]
    count = tall // members
    out = jnp.zeros_like(planes[0])
    for n, plane in enumerate(planes):
        moved = pltpu.roll(plane, n * count, 0) if n else plane
        out = jnp.where(where_block(plane.shape, count, member + n, members), moved, out)
    return out


def from_shares(shares, members, n):
    tall = shares[0][1].shape[0]
    count = tall // members
    out = jnp.zeros_like(shares[0][1])
    for member, share in shares:
        out = jnp.where(where_block(share.shape, count, member + n, members), share, out)
    return pltpu.roll(out, tall - n * count, 0) if n else out


def send_rows(matrix_ref, field, lines, out_ref):
    owners = out_ref.shape[0]
    rows = matrix_ref.shape[0]
    tall = field[0][0].shape[0]
    block = lax.axis_index("dp")
    members = lax.axis_size("dp")
    gravity_rows = block < members * 3 // 4
    chosen = [jnp.where(gravity_rows, d, s) for d, s in zip(field[0], field[1])]
    vector = spread(chosen, LANES).astype(jnp.bfloat16)
    eye = lax.broadcasted_iota(jnp.int32, (LANES, LANES), 0) == lax.broadcasted_iota(
        jnp.int32, (LANES, LANES), 1
    )
    product = lax.dot_general(
        matrix_ref[...], vector, (((1,), (1,)), ((), ())), preferred_element_type=jnp.float32
    )
    pieces = [
        jnp.sum(
            jnp.where(eye, product[b * LANES : (b + 1) * LANES], 0.0), axis=0, keepdims=True
        )
        for b in range(rows // LANES)
    ]
    edges = [field[0][0], field[1][0], field[0][-1], field[1][-1]]
    pieces.append(share_of(edges, block, members))
    pieces += lines
    pieces.append(jnp.zeros((SUBLANES - len(lines), LANES), jnp.float32))
    message = jnp.concatenate(pieces, axis=0)
    for j in range(owners):
        out_ref[j] = message


def load_layers(ref):
    layers, width = ref.shape
    return [
        jnp.concatenate([ref[i : i + 1, t : t + LANES] for t in range(0, width, LANES)], axis=0)
        for i in range(layers)
    ]


def load_wide(ref):
    return [load_layers(ref.at[f]) for f in range(2)]


def store_wide(ref, field):
    for f in range(2):
        for i in range(ref.shape[1]):
            for t in range(ref.shape[2] // LANES):
                ref[f, i : i + 1, t * LANES : (t + 1) * LANES] = field[f][i][t : t + 1]


def start_kernel(matrix_ref, model_ref, out_ref):
    send_rows(matrix_ref, load_wide(model_ref), [], out_ref)


def rows_kernel(
    matrix_ref, got_ref, weight_ref, observed_ref, out_ref, *, subtract, tall
):
    rank = lax.axis_index("mp")
    member = lax.axis_index("dp")
    members = lax.axis_size("dp")
    owners = got_ref.shape[0]
    rows, cells = matrix_ref.shape
    blocks = rows // LANES
    values = got_ref[0, 0:blocks]
    for j in range(1, owners):
        values = values + got_ref[j, 0:blocks]
    if subtract:
        values = values - observed_ref[...]
    scaled = (weight_ref[...] * values).astype(jnp.bfloat16).astype(jnp.float32)
    weighed = jnp.sum(values * scaled, axis=0, keepdims=True)
    vector = spread([scaled], 2 * SUBLANES).astype(jnp.bfloat16)
    columns = jnp.dot(vector, matrix_ref[...], preferred_element_type=jnp.float32)
    pieces = [columns[0:1, t * LANES : (t + 1) * LANES] for t in range(cells // LANES)]
    count = tall // members
    shares = [got_ref[j, blocks : blocks + tall] for j in range(owners)]
    held = [where_block(shares[0].shape, count, member + n, members) for n in range(4)]
    lower = held[0] | held[1]
    upper = held[2] | held[3]
    cross = None
    for j in range(owners - 1):
        term = shares[j] * pltpu.roll(shares[j + 1], 2 * count, 0)
        cross = term if cross is None else cross + term
    cross = jnp.sum(jnp.where(upper, cross, 0.0), axis=0, keepdims=True)
    weighed = weighed - 2.0 * SMOOTHING * cross
    down = jnp.maximum(rank - 1, 0)
    up = jnp.minimum(rank + 1, owners - 1)
    above = jnp.where(lower & (rank < owners - 1), got_ref[up, blocks : blocks + tall], 0.0)
    below = jnp.where(upper & (rank > 0), got_ref[down, blocks : blocks + tall], 0.0)
    pieces += [above + below, weighed, jnp.zeros((SUBLANES - 1, LANES), jnp.float32)]
    out_ref[...] = jnp.concatenate(pieces, axis=0)


def gathered(part_refs, inner_ref, mask_ref):
    layers, tall = inner_ref.shape[1:3]
    cells = layers * tall
    members = len(part_refs)
    sources = [lax.axis_index("dp") ^ s for s in range(members)]
    gravity = [q < members * 3 // 4 for q in sources]
    parts = [ref[0:cells] for ref in part_refs]
    data = [
        tree_sum([jnp.where(g, p, 0.0) for g, p in zip(gravity, parts)]),
        tree_sum([jnp.where(g, 0.0, p) for g, p in zip(gravity, parts)]),
    ]
    shares = [(q, ref[cells : cells + tall]) for q, ref in zip(sources, part_refs)]
    image = [[], []]
    for f in range(2):
        above = from_shares(shares, members, f)
        below = from_shares(shares, members, 2 + f)
        for i in range(layers):
            regular = inner_ref[f, i]
            if i == 0:
                regular = regular - SMOOTHING * below
            if i == layers - 1:
                regular = regular - SMOOTHING * above
            image[f].append(mask_ref[f, i] * (data[f][i * tall : (i + 1) * tall] + regular))
    return image


def first_kernel(matrix_ref, *refs, count):
    part_refs = refs[:count]
    model_ref, weight_ref, active_ref, out_ref, residual_ref, inner_ref = refs[count : count + 6]
    smooth_ref, mask_ref, held = refs[count + 6 :]
    layers = model_ref.shape[1]
    smooth_weight = load_layers(weight_ref)
    for i in range(layers):
        smooth_ref[i] = smooth_weight[i]
    store(mask_ref, mapped(lambda a: 1.0 - a.astype(jnp.float32), load_wide(active_ref)))
    store(held, operate_inner(load_wide(model_ref), smooth_weight))
    image = gathered(part_refs, held, mask_ref)
    residual = mapped(lambda a: -a, image)
    inner = operate_inner(residual, smooth_weight)
    store(residual_ref, residual)
    store(inner_ref, inner)
    lines = [dot_line(residual, residual), dot_line(residual, inner)]
    send_rows(matrix_ref, residual, lines, out_ref)


def cells_kernel(matrix_ref, *refs, count, base, begin, final):
    part_refs = refs[:count]
    got_ref, smooth_ref, mask_ref, residual_in, inner_in = refs[count : count + 5]
    refs = refs[count + 5 :]
    if not begin:
        direction_in, imaged_in, solution_in, norms_in = refs[:4]
        refs = refs[4:]
    solution_ref, residual_ref = refs[:2]
    owners = got_ref.shape[0]
    layers, tall = inner_in.shape[1:3]
    cells = layers * tall
    residual = load(residual_in)
    image = gathered(part_refs, inner_in, mask_ref)
    at = base + tall
    sums = got_ref[0, at : at + SUBLANES]
    for j in range(1, owners):
        sums = sums + got_ref[j, at : at + SUBLANES]
    at = cells + tall
    weighed = tree_sum([ref[at : at + 1] for ref in part_refs])
    line = weighed + sums[1:2]
    norm_now = full(sums[0:1])
    curvature = full(line)
    if begin:
        direction, imaged = residual, image
    else:
        ratio = norm_now / norms_in[0:1, 0:1]
        curvature = curvature + ratio * (2.0 * full(sums[2:3]) + ratio * norms_in[1:2, 0:1])
        direction = mapped(lambda r, d: r + ratio * d, residual, load(direction_in))
        imaged = mapped(lambda r, d: r + ratio * d, image, load(imaged_in))
    step_len = norm_now / curvature
    if begin:
        update = mapped(lambda d: step_len * d, direction)
    else:
        update = mapped(lambda x, d: x + step_len * d, load(solution_in), direction)
    residual = mapped(lambda r, s: r - step_len * s, residual, imaged)
    if final:
        store_wide(solution_ref, update)
        store_wide(residual_ref, residual)
        return
    store(solution_ref, update)
    store(residual_ref, residual)
    direction_ref, imaged_ref, norms_ref, inner_ref, out_ref = refs[2:]
    store(direction_ref, direction)
    store(imaged_ref, imaged)
    norms_ref[0:1] = jnp.broadcast_to(norm_now, (1, LANES))
    norms_ref[1:2] = jnp.broadcast_to(curvature, (1, LANES))
    inner = operate_inner(residual, [smooth_ref[i] for i in range(layers)])
    store(inner_ref, inner)
    lines = [dot_line(residual, residual), dot_line(residual, inner), dot_line(residual, imaged)]
    send_rows(matrix_ref, residual, lines, out_ref)


def local(sensitivity, observed, row_weight, model, smooth_weight, active):
    rows = sensitivity.shape[0]
    matrix = sensitivity.reshape(rows, -1)
    layers, width = smooth_weight.shape
    tall = width // LANES
    owners = lax.axis_size("mp")
    blocks = lax.axis_size("dp")
    base = rows // LANES

    weight = row_weight.reshape(base, LANES)
    target = observed.reshape(base, LANES)

    cell = jax.ShapeDtypeStruct((2, layers, tall, LANES), jnp.float32)
    field = jax.ShapeDtypeStruct(cell.shape[1:], jnp.float32)
    wide = jax.ShapeDtypeStruct(model.shape, jnp.float32)
    if tall % blocks or blocks < 4:
        raise ValueError("boundary shares")
    message = jax.ShapeDtypeStruct((owners, base + tall + SUBLANES, LANES), jnp.float32)
    columns = jax.ShapeDtypeStruct(((layers + 1) * tall + SUBLANES, LANES), jnp.float32)
    norms = jax.ShapeDtypeStruct((2, LANES), jnp.float32)
    vmem = pl.BlockSpec(memory_space=pltpu.VMEM)

    def call(kernel, out_shape, *operands, name, scratch=()):
        held = pltpu.with_memory_space_constraint(matrix, pltpu.VMEM)
        return pl.pallas_call(
            kernel,
            out_shape=out_shape,
            in_specs=[vmem] * (1 + len(operands)),
            out_specs=jax.tree.map(lambda _: vmem, out_shape),
            scratch_shapes=scratch,
            compiler_params=pltpu.CompilerParams(vmem_limit_bytes=KERNEL_VMEM),
            name=name,
        )(held, *operands)

    def across(sent):
        return lax.all_to_all(sent, "mp", 0, 0, tiled=True)

    def along(got, subtract):
        sent = call(
            functools.partial(rows_kernel, subtract=subtract, tall=tall),
            columns,
            got,
            weight,
            target,
            name="rows",
        )
        return [sent] + [
            lax.ppermute(sent, "dp", [(i, i ^ s) for i in range(blocks)])
            for s in range(1, blocks)
        ]

    got = across(call(start_kernel, message, model, name="start"))
    parts = along(got, True)
    sent, residual, inner, smooth, mask = call(
        functools.partial(first_kernel, count=blocks),
        (message, cell, cell, field, cell),
        *parts,
        model,
        smooth_weight,
        active,
        name="first",
        scratch=[pltpu.VMEM(cell.shape, jnp.float32)],
    )
    carried = ()
    for step in range(ITERS):
        got = across(sent)
        parts = along(got, False)
        final = step == ITERS - 1
        outs = (wide, wide) if final else (cell, cell, cell, cell, norms, cell, message)
        result = call(
            functools.partial(
                cells_kernel, count=blocks, base=base, begin=step == 0, final=final
            ),
            outs,
            *parts,
            got,
            smooth,
            mask,
            residual,
            inner,
            *carried,
            name="cells",
        )
        if final:
            update, residual = result
        else:
            update, residual, direction, imaged, scalars, inner, sent = result
            carried = (direction, imaged, update, scalars)
    return (update, residual)


def solution(mesh):
    return jax.shard_map(
        local,
        mesh=mesh,
        in_specs=(
            P("dp", "mp", None),
            P("dp"),
            P("dp"),
            P(None, "mp", None),
            P("mp", None),
            P(None, "mp", None),
        ),
        out_specs=(P(None, "mp", None), P(None, "mp", None)),
        check_vma=False,
    )
```

```python
import functools

import jax
import jax.numpy as jnp
from jax import lax
from jax.experimental import pallas as pl
from jax.experimental.pallas import tpu as pltpu
from jax.sharding import PartitionSpec as P

GZ = 16
ITERS = 4


SMOOTHING = 0.25
COUPLING = 0.5
LANES = 128
SUBLANES = 8
KERNEL_VMEM = 16 * 1024 * 1024


def tree_sum(parts):
    while len(parts) > 1:
        parts = [parts[i] + parts[i + 1] for i in range(0, len(parts), 2)]
    return parts[0]


def inner_sum(plane):
    tall = plane.shape[0]
    lane = lax.broadcasted_iota(jnp.int32, plane.shape, 1)
    line = lax.broadcasted_iota(jnp.int32, plane.shape, 0)
    position = lane % GZ
    later = jnp.where(position != GZ - 1, pltpu.roll(plane, LANES - 1, 1), 0.0)
    earlier = jnp.where(position != 0, pltpu.roll(plane, 1, 1), 0.0)
    ahead = pltpu.roll(plane, LANES - GZ, 1)
    over = jnp.where(line < tall - 1, pltpu.roll(ahead, tall - 1, 0), 0.0)
    ahead = jnp.where(lane < LANES - GZ, ahead, over)
    behind = pltpu.roll(plane, GZ, 1)
    under = jnp.where(line > 0, pltpu.roll(behind, 1, 0), 0.0)
    behind = jnp.where(lane >= GZ, behind, under)
    return later + earlier + ahead + behind


def operate_inner(field, smooth_weight):
    layers = len(field[0])
    out = [[], []]
    for f in range(2):
        for i in range(layers):
            own = field[f][i]
            beside = inner_sum(own)
            if i:
                beside = beside + field[f][i - 1]
            if i < layers - 1:
                beside = beside + field[f][i + 1]
            out[f].append(
                smooth_weight[i] * own
                + SMOOTHING * (6.0 * own - beside)
                + COUPLING * (own - field[1 - f][i])
            )
    return out


def load(ref):
    return [[ref[f, i] for i in range(ref.shape[1])] for f in range(2)]


def store(ref, field):
    for f in range(2):
        for i in range(ref.shape[1]):
            ref[f, i] = field[f][i]


def mapped(op, *fields):
    return [[op(*(x[f][i] for x in fields)) for i in range(len(fields[0][0]))] for f in range(2)]


def dot_line(one, two):
    total = None
    for f in range(2):
        for i in range(len(one[0])):
            term = one[f][i] * two[f][i]
            total = term if total is None else total + term
    return jnp.sum(total, axis=0, keepdims=True)


def full(line):
    return jnp.sum(line, axis=1, keepdims=True)


def spread(planes, count):
    return jnp.concatenate(
        [
            jnp.broadcast_to(plane[t : t + 1], (count, LANES))
            for plane in planes
            for t in range(plane.shape[0])
        ],
        axis=1,
    )


def where_block(shape, count, block, members):
    line = lax.broadcasted_iota(jnp.int32, shape, 0)
    return line // count == lax.rem(block, jnp.int32(members))


def share_of(planes, member, members):
    tall = planes[0].shape[0]
    count = tall // members
    out = jnp.zeros_like(planes[0])
    for n, plane in enumerate(planes):
        moved = pltpu.roll(plane, n * count, 0) if n else plane
        out = jnp.where(where_block(plane.shape, count, member + n, members), moved, out)
    return out


def from_shares(shares, members, n):
    tall = shares[0][1].shape[0]
    count = tall // members
    out = jnp.zeros_like(shares[0][1])
    for member, share in shares:
        out = jnp.where(where_block(share.shape, count, member + n, members), share, out)
    return pltpu.roll(out, tall - n * count, 0) if n else out


def send_rows(matrix_ref, field, lines, out_ref, ready=None):
    owners = out_ref.shape[0]
    rows = matrix_ref.shape[0]
    tall = field[0][0].shape[0]
    member = lax.axis_index("dp")
    members = lax.axis_size("dp")
    gravity_rows = member < members * 3 // 4
    chosen = [jnp.where(gravity_rows, d, s) for d, s in zip(field[0], field[1])]
    eye = lax.broadcasted_iota(jnp.int32, (LANES, LANES), 0) == lax.broadcasted_iota(
        jnp.int32, (LANES, LANES), 1
    )
    lines_in = [plane[t : t + 1] for plane in chosen for t in range(tall)]
    pieces = []
    for b in range(rows // LANES):
        if ready is not None:
            ready(b)
        total = None
        for t, line in enumerate(lines_in):
            block = matrix_ref[b * LANES : (b + 1) * LANES, t * LANES : (t + 1) * LANES]
            term = block.astype(jnp.float32) * line
            total = term if total is None else total + term
        column = jnp.sum(total, axis=1, keepdims=True)
        pieces.append(jnp.sum(jnp.where(eye, column, 0.0), axis=0, keepdims=True))
    edges = [field[0][0], field[1][0], field[0][-1], field[1][-1]]
    pieces.append(share_of(edges, member, members))
    pieces += lines
    pieces.append(jnp.zeros((SUBLANES - len(lines), LANES), jnp.float32))
    message = jnp.concatenate(pieces, axis=0)
    for j in range(owners):
        out_ref[j] = message


def load_layers(ref):
    layers, width = ref.shape
    return [
        jnp.concatenate([ref[i : i + 1, t : t + LANES] for t in range(0, width, LANES)], axis=0)
        for i in range(layers)
    ]


def load_wide(ref):
    return [load_layers(ref.at[f]) for f in range(2)]


def store_wide(ref, field):
    for f in range(2):
        for i in range(ref.shape[1]):
            for t in range(ref.shape[2] // LANES):
                ref[f, i : i + 1, t * LANES : (t + 1) * LANES] = field[f][i][t : t + 1]


def start_kernel(raw_ref, far_ref, matrix_ref, out_ref, chunks, arrived, model_ref, came):
    def fetch(b):
        return pltpu.make_async_copy(
            raw_ref.at[pl.ds(b * LANES, LANES)], chunks.at[b], arrived.at[b]
        )

    model_copy = pltpu.make_async_copy(far_ref, model_ref, came)
    model_copy.start()
    for b in range(chunks.shape[0]):
        fetch(b).start()

    def ready(b):
        fetch(b).wait()
        block = chunks[b]
        matrix_ref[b * LANES : (b + 1) * LANES] = block.reshape(LANES, -1)

    model_copy.wait()
    send_rows(matrix_ref, load_wide(model_ref), [], out_ref, ready)


def rows_kernel(
    matrix_ref, got_ref, weight_ref, observed_ref, out_ref, *, subtract, tall
):
    rank = lax.axis_index("mp")
    member = lax.axis_index("dp")
    members = lax.axis_size("dp")
    owners = got_ref.shape[0]
    rows, cells = matrix_ref.shape
    blocks = rows // LANES
    values = got_ref[0, 0:blocks]
    for j in range(1, owners):
        values = values + got_ref[j, 0:blocks]
    if subtract:
        values = values - observed_ref[...]
    scaled = (weight_ref[...] * values).astype(jnp.bfloat16).astype(jnp.float32)
    weighed = jnp.sum(values * scaled, axis=0, keepdims=True)
    vector = spread([scaled], 2 * SUBLANES).astype(jnp.bfloat16)
    columns = jnp.dot(vector, matrix_ref[...], preferred_element_type=jnp.float32)
    pieces = [columns[0:1, t * LANES : (t + 1) * LANES] for t in range(cells // LANES)]
    count = tall // members
    shares = [got_ref[j, blocks : blocks + tall] for j in range(owners)]
    held = [where_block(shares[0].shape, count, member + n, members) for n in range(4)]
    lower = held[0] | held[1]
    upper = held[2] | held[3]
    cross = None
    for j in range(owners - 1):
        term = shares[j] * pltpu.roll(shares[j + 1], 2 * count, 0)
        cross = term if cross is None else cross + term
    cross = jnp.sum(jnp.where(upper, cross, 0.0), axis=0, keepdims=True)
    weighed = weighed - 2.0 * SMOOTHING * cross
    down = jnp.maximum(rank - 1, 0)
    up = jnp.minimum(rank + 1, owners - 1)
    above = jnp.where(lower & (rank < owners - 1), got_ref[up, blocks : blocks + tall], 0.0)
    below = jnp.where(upper & (rank > 0), got_ref[down, blocks : blocks + tall], 0.0)
    pieces += [above + below, weighed, jnp.zeros((SUBLANES - 1, LANES), jnp.float32)]
    out_ref[...] = jnp.concatenate(pieces, axis=0)


def gathered(part_refs, inner_ref, mask_ref):
    layers, tall = inner_ref.shape[1:3]
    cells = layers * tall
    members = len(part_refs)
    sources = [lax.axis_index("dp") ^ s for s in range(members)]
    gravity = [q < members * 3 // 4 for q in sources]
    parts = [ref[0:cells] for ref in part_refs]
    data = [
        tree_sum([jnp.where(g, p, 0.0) for g, p in zip(gravity, parts)]),
        tree_sum([jnp.where(g, 0.0, p) for g, p in zip(gravity, parts)]),
    ]
    shares = [(q, ref[cells : cells + tall]) for q, ref in zip(sources, part_refs)]
    image = [[], []]
    for f in range(2):
        above = from_shares(shares, members, f)
        below = from_shares(shares, members, 2 + f)
        for i in range(layers):
            regular = inner_ref[f, i]
            if i == 0:
                regular = regular - SMOOTHING * below
            if i == layers - 1:
                regular = regular - SMOOTHING * above
            image[f].append(mask_ref[f, i] * (data[f][i * tall : (i + 1) * tall] + regular))
    return image


def first_kernel(matrix_ref, *refs, count):
    part_refs = refs[:count]
    model_ref, weight_ref, active_ref, out_ref, residual_ref, inner_ref = refs[count : count + 6]
    smooth_ref, mask_ref, held = refs[count + 6 :]
    layers = model_ref.shape[1]
    smooth_weight = load_layers(weight_ref)
    for i in range(layers):
        smooth_ref[i] = smooth_weight[i]
    store(mask_ref, mapped(lambda a: 1.0 - a.astype(jnp.float32), load_wide(active_ref)))
    store(held, operate_inner(load_wide(model_ref), smooth_weight))
    image = gathered(part_refs, held, mask_ref)
    residual = mapped(lambda a: -a, image)
    inner = operate_inner(residual, smooth_weight)
    store(residual_ref, residual)
    store(inner_ref, inner)
    lines = [dot_line(residual, residual), dot_line(residual, inner)]
    send_rows(matrix_ref, residual, lines, out_ref)


def cells_kernel(matrix_ref, *refs, count, base, begin, final):
    part_refs = refs[:count]
    got_ref, smooth_ref, mask_ref, residual_in, inner_in = refs[count : count + 5]
    refs = refs[count + 5 :]
    if not begin:
        direction_in, imaged_in, solution_in, norms_in = refs[:4]
        refs = refs[4:]
    solution_ref, residual_ref = refs[:2]
    owners = got_ref.shape[0]
    layers, tall = inner_in.shape[1:3]
    cells = layers * tall
    residual = load(residual_in)
    image = gathered(part_refs, inner_in, mask_ref)
    at = base + tall
    sums = got_ref[0, at : at + SUBLANES]
    for j in range(1, owners):
        sums = sums + got_ref[j, at : at + SUBLANES]
    at = cells + tall
    weighed = tree_sum([ref[at : at + 1] for ref in part_refs])
    line = weighed + sums[1:2]
    norm_now = full(sums[0:1])
    curvature = full(line)
    if begin:
        direction, imaged = residual, image
    else:
        ratio = norm_now / norms_in[0:1, 0:1]
        curvature = curvature + ratio * (2.0 * full(sums[2:3]) + ratio * norms_in[1:2, 0:1])
        direction = mapped(lambda r, d: r + ratio * d, residual, load(direction_in))
        imaged = mapped(lambda r, d: r + ratio * d, image, load(imaged_in))
    step_len = norm_now / curvature
    if begin:
        update = mapped(lambda d: step_len * d, direction)
    else:
        update = mapped(lambda x, d: x + step_len * d, load(solution_in), direction)
    residual = mapped(lambda r, s: r - step_len * s, residual, imaged)
    if final:
        store_wide(solution_ref, update)
        store_wide(residual_ref, residual)
        return
    store(solution_ref, update)
    store(residual_ref, residual)
    direction_ref, imaged_ref, norms_ref, inner_ref, out_ref = refs[2:]
    store(direction_ref, direction)
    store(imaged_ref, imaged)
    norms_ref[0:1] = jnp.broadcast_to(norm_now, (1, LANES))
    norms_ref[1:2] = jnp.broadcast_to(curvature, (1, LANES))
    inner = operate_inner(residual, [smooth_ref[i] for i in range(layers)])
    store(inner_ref, inner)
    lines = [dot_line(residual, residual), dot_line(residual, inner), dot_line(residual, imaged)]
    send_rows(matrix_ref, residual, lines, out_ref)


def local(sensitivity, observed, row_weight, model, smooth_weight, active):
    rows = sensitivity.shape[0]
    layers, width = smooth_weight.shape
    tall = width // LANES
    owners = lax.axis_size("mp")
    blocks = lax.axis_size("dp")
    base = rows // LANES

    weight = row_weight.reshape(base, LANES)
    target = observed.reshape(base, LANES)

    cell = jax.ShapeDtypeStruct((2, layers, tall, LANES), jnp.float32)
    field = jax.ShapeDtypeStruct(cell.shape[1:], jnp.float32)
    wide = jax.ShapeDtypeStruct(model.shape, jnp.float32)
    if tall % blocks or blocks < 4:
        raise ValueError("boundary shares")
    message = jax.ShapeDtypeStruct((owners, base + tall + SUBLANES, LANES), jnp.float32)
    columns = jax.ShapeDtypeStruct(((layers + 1) * tall + SUBLANES, LANES), jnp.float32)
    norms = jax.ShapeDtypeStruct((2, LANES), jnp.float32)
    vmem = pl.BlockSpec(memory_space=pltpu.VMEM)

    def call(kernel, out_shape, *operands, name, scratch=()):
        return pl.pallas_call(
            kernel,
            out_shape=out_shape,
            in_specs=[vmem] * len(operands),
            out_specs=jax.tree.map(lambda _: vmem, out_shape),
            scratch_shapes=scratch,
            compiler_params=pltpu.CompilerParams(vmem_limit_bytes=KERNEL_VMEM),
            name=name,
        )(*operands)

    def across(sent):
        return lax.all_to_all(sent, "mp", 0, 0, tiled=True)

    def along(got, subtract):
        sent = call(
            functools.partial(rows_kernel, subtract=subtract, tall=tall),
            columns,
            matrix,
            got,
            weight,
            target,
            name="rows",
        )
        return [sent] + [
            lax.ppermute(sent, "dp", [(i, i ^ s) for i in range(blocks)])
            for s in range(1, blocks)
        ]

    matrix, sent = pl.pallas_call(
        start_kernel,
        out_shape=(jax.ShapeDtypeStruct((rows, layers * width), sensitivity.dtype), message),
        in_specs=[pl.BlockSpec(memory_space=pltpu.HBM)] * 2,
        out_specs=(vmem, vmem),
        scratch_shapes=[
            pltpu.VMEM((base, LANES) + sensitivity.shape[1:], sensitivity.dtype),
            pltpu.SemaphoreType.DMA((base,)),
            pltpu.VMEM(model.shape, jnp.float32),
            pltpu.SemaphoreType.DMA,
        ],
        compiler_params=pltpu.CompilerParams(vmem_limit_bytes=KERNEL_VMEM),
        name="start",
    )(*[pltpu.with_memory_space_constraint(x, pltpu.HBM) for x in (sensitivity, model)])
    matrix = pltpu.with_memory_space_constraint(matrix, pltpu.VMEM)
    got = across(sent)
    parts = along(got, True)
    sent, residual, inner, smooth, mask = call(
        functools.partial(first_kernel, count=blocks),
        (message, cell, cell, field, cell),
        matrix,
        *parts,
        model,
        smooth_weight,
        active,
        name="first",
        scratch=[pltpu.VMEM(cell.shape, jnp.float32)],
    )
    carried = ()
    for step in range(ITERS):
        got = across(sent)
        parts = along(got, False)
        final = step == ITERS - 1
        outs = (wide, wide) if final else (cell, cell, cell, cell, norms, cell, message)
        result = call(
            functools.partial(
                cells_kernel, count=blocks, base=base, begin=step == 0, final=final
            ),
            outs,
            matrix,
            *parts,
            got,
            smooth,
            mask,
            residual,
            inner,
            *carried,
            name="cells",
        )
        if final:
            update, residual = result
        else:
            update, residual, direction, imaged, scalars, inner, sent = result
            carried = (direction, imaged, update, scalars)
    return (update, residual)


def solution(mesh):
    return jax.shard_map(
        local,
        mesh=mesh,
        in_specs=(
            P("dp", "mp", None),
            P("dp"),
            P("dp"),
            P(None, "mp", None),
            P("mp", None),
            P(None, "mp", None),
        ),
        out_specs=(P(None, "mp", None), P(None, "mp", None)),
        check_vma=False,
    )
```

```python
import functools

import jax
import jax.numpy as jnp
from jax import lax
from jax.experimental import pallas as pl
from jax.experimental.pallas import tpu as pltpu
from jax.sharding import PartitionSpec as P

GZ = 16
ITERS = 4


SMOOTHING = 0.25
COUPLING = 0.5
LANES = 128
SUBLANES = 8
SCALARS = 3
CHUNK = 64
IN_FLIGHT = 6
KERNEL_VMEM = 16 * 1024 * 1024


def tree_sum(parts):
    while len(parts) > 1:
        parts = [parts[i] + parts[i + 1] for i in range(0, len(parts), 2)]
    return parts[0]


def inner_sum(plane):
    tall = plane.shape[0]
    lane = lax.broadcasted_iota(jnp.int32, plane.shape, 1)
    line = lax.broadcasted_iota(jnp.int32, plane.shape, 0)
    position = lane % GZ
    later = jnp.where(position != GZ - 1, pltpu.roll(plane, LANES - 1, 1), 0.0)
    earlier = jnp.where(position != 0, pltpu.roll(plane, 1, 1), 0.0)
    ahead = pltpu.roll(plane, LANES - GZ, 1)
    over = jnp.where(line < tall - 1, pltpu.roll(ahead, tall - 1, 0), 0.0)
    ahead = jnp.where(lane < LANES - GZ, ahead, over)
    behind = pltpu.roll(plane, GZ, 1)
    under = jnp.where(line > 0, pltpu.roll(behind, 1, 0), 0.0)
    behind = jnp.where(lane >= GZ, behind, under)
    return later + earlier + ahead + behind


def operate_inner(field, smooth_weight):
    layers = len(field[0])
    out = [[], []]
    for f in range(2):
        for i in range(layers):
            own = field[f][i]
            beside = inner_sum(own)
            if i:
                beside = beside + field[f][i - 1]
            if i < layers - 1:
                beside = beside + field[f][i + 1]
            out[f].append(
                smooth_weight[i] * own
                + SMOOTHING * (6.0 * own - beside)
                + COUPLING * (own - field[1 - f][i])
            )
    return out


def load(ref):
    return [[ref[f, i] for i in range(ref.shape[1])] for f in range(2)]


def store(ref, field):
    for f in range(2):
        for i in range(ref.shape[1]):
            ref[f, i] = field[f][i]


def mapped(op, *fields):
    return [[op(*(x[f][i] for x in fields)) for i in range(len(fields[0][0]))] for f in range(2)]


def dot_line(one, two):
    total = None
    for f in range(2):
        for i in range(len(one[0])):
            term = one[f][i] * two[f][i]
            total = term if total is None else total + term
    return jnp.sum(total, axis=0, keepdims=True)


def full(line):
    return jnp.sum(line, axis=1, keepdims=True)


def spread(planes, count):
    return jnp.concatenate(
        [
            jnp.broadcast_to(plane[t : t + 1], (count, LANES))
            for plane in planes
            for t in range(plane.shape[0])
        ],
        axis=1,
    )


def where_block(shape, count, block, members):
    line = lax.broadcasted_iota(jnp.int32, shape, 0)
    return line // count == lax.rem(block, jnp.int32(members))


def share_of(planes, member, members):
    tall = planes[0].shape[0]
    count = tall // members
    out = jnp.zeros_like(planes[0])
    for n, plane in enumerate(planes):
        moved = pltpu.roll(plane, n * count, 0) if n else plane
        out = jnp.where(where_block(plane.shape, count, member + n, members), moved, out)
    return out


def from_shares(shares, members, n):
    tall = shares[0][1].shape[0]
    count = tall // members
    out = jnp.zeros_like(shares[0][1])
    for member, share in shares:
        out = jnp.where(where_block(share.shape, count, member + n, members), share, out)
    return pltpu.roll(out, tall - n * count, 0) if n else out


def send_rows(matrix_ref, field, lines, out_ref, ready=None):
    owners = out_ref.shape[0]
    rows = matrix_ref.shape[0]
    tall = field[0][0].shape[0]
    member = lax.axis_index("dp")
    members = lax.axis_size("dp")
    gravity_rows = member < members * 3 // 4
    chosen = [jnp.where(gravity_rows, d, s) for d, s in zip(field[0], field[1])]
    eye = lax.broadcasted_iota(jnp.int32, (LANES, LANES), 0) == lax.broadcasted_iota(
        jnp.int32, (LANES, LANES), 1
    )
    lines_in = [plane[t : t + 1] for plane in chosen for t in range(tall)]
    pieces = []
    for b in range(rows // LANES):
        if ready is not None:
            ready(b)
        total = None
        for t, line in enumerate(lines_in):
            block = matrix_ref[b * LANES : (b + 1) * LANES, t * LANES : (t + 1) * LANES]
            term = block.astype(jnp.float32) * line
            total = term if total is None else total + term
        column = jnp.sum(total, axis=1, keepdims=True)
        pieces.append(jnp.sum(jnp.where(eye, column, 0.0), axis=0, keepdims=True))
    edges = [field[0][0], field[1][0], field[0][-1], field[1][-1]]
    pieces.append(share_of(edges, member, members))
    pieces += lines
    message = jnp.concatenate(pieces, axis=0)
    for j in range(owners):
        out_ref[j, 0 : message.shape[0], 0] = message


def load_layers(ref):
    layers, width = ref.shape
    return [
        jnp.concatenate([ref[i : i + 1, t : t + LANES] for t in range(0, width, LANES)], axis=0)
        for i in range(layers)
    ]


def load_wide(ref):
    return [load_layers(ref.at[f]) for f in range(2)]


def store_wide(ref, field):
    for f in range(2):
        for i in range(ref.shape[1]):
            for t in range(ref.shape[2] // LANES):
                ref[f, i : i + 1, t * LANES : (t + 1) * LANES] = field[f][i][t : t + 1]


def start_kernel(raw_ref, far_ref, matrix_ref, out_ref, chunks, arrived, model_ref, came):
    count, height = chunks.shape[:2]

    def fetch(n):
        return pltpu.make_async_copy(
            raw_ref.at[pl.ds(n * height, height)], chunks.at[n], arrived.at[n]
        )

    model_copy = pltpu.make_async_copy(far_ref, model_ref, came)
    model_copy.start()
    for n in range(min(IN_FLIGHT, count)):
        fetch(n).start()

    def ready(b):
        for n in range(b * LANES // height, (b + 1) * LANES // height):
            fetch(n).wait()
            if n + IN_FLIGHT < count:
                fetch(n + IN_FLIGHT).start()
            block = chunks[n]
            matrix_ref[n * height : (n + 1) * height] = block.reshape(height, -1)

    model_copy.wait()
    send_rows(matrix_ref, load_wide(model_ref), [], out_ref, ready)


def rows_kernel(
    matrix_ref, got_ref, weight_ref, observed_ref, out_ref, *, subtract, tall
):
    rank = lax.axis_index("mp")
    member = lax.axis_index("dp")
    members = lax.axis_size("dp")
    owners = got_ref.shape[0]
    rows, cells = matrix_ref.shape
    blocks = rows // LANES
    values = got_ref[0, 0:blocks, 0]
    for j in range(1, owners):
        values = values + got_ref[j, 0:blocks, 0]
    if subtract:
        values = values - observed_ref[...]
    scaled = (weight_ref[...] * values).astype(jnp.bfloat16).astype(jnp.float32)
    weighed = jnp.sum(values * scaled, axis=0, keepdims=True)
    vector = spread([scaled], 2 * SUBLANES).astype(jnp.bfloat16)
    columns = jnp.dot(vector, matrix_ref[...], preferred_element_type=jnp.float32)
    pieces = [columns[0:1, t * LANES : (t + 1) * LANES] for t in range(cells // LANES)]
    count = tall // members
    shares = [got_ref[j, blocks : blocks + tall, 0] for j in range(owners)]
    held = [where_block(shares[0].shape, count, member + n, members) for n in range(4)]
    lower = held[0] | held[1]
    upper = held[2] | held[3]
    cross = None
    for j in range(owners - 1):
        term = shares[j] * pltpu.roll(shares[j + 1], 2 * count, 0)
        cross = term if cross is None else cross + term
    cross = jnp.sum(jnp.where(upper, cross, 0.0), axis=0, keepdims=True)
    weighed = weighed - 2.0 * SMOOTHING * cross
    down = jnp.maximum(rank - 1, 0)
    up = jnp.minimum(rank + 1, owners - 1)
    above = jnp.where(lower & (rank < owners - 1), got_ref[up, blocks : blocks + tall, 0], 0.0)
    below = jnp.where(upper & (rank > 0), got_ref[down, blocks : blocks + tall, 0], 0.0)
    pieces += [above + below, weighed, jnp.zeros((SUBLANES - 1, LANES), jnp.float32)]
    out_ref[...] = jnp.concatenate(pieces, axis=0)


def gathered(part_refs, inner_ref, mask_ref):
    layers, tall = inner_ref.shape[1:3]
    cells = layers * tall
    members = len(part_refs)
    sources = [lax.axis_index("dp") ^ s for s in range(members)]
    gravity = [q < members * 3 // 4 for q in sources]
    parts = [ref[0:cells] for ref in part_refs]
    data = [
        tree_sum([jnp.where(g, p, 0.0) for g, p in zip(gravity, parts)]),
        tree_sum([jnp.where(g, 0.0, p) for g, p in zip(gravity, parts)]),
    ]
    shares = [(q, ref[cells : cells + tall]) for q, ref in zip(sources, part_refs)]
    image = [[], []]
    for f in range(2):
        above = from_shares(shares, members, f)
        below = from_shares(shares, members, 2 + f)
        for i in range(layers):
            regular = inner_ref[f, i]
            if i == 0:
                regular = regular - SMOOTHING * below
            if i == layers - 1:
                regular = regular - SMOOTHING * above
            image[f].append(mask_ref[f, i] * (data[f][i * tall : (i + 1) * tall] + regular))
    return image


def first_kernel(matrix_ref, *refs, count):
    part_refs = refs[:count]
    model_ref, weight_ref, active_ref, out_ref, residual_ref, inner_ref = refs[count : count + 6]
    smooth_ref, mask_ref, held = refs[count + 6 :]
    layers = model_ref.shape[1]
    smooth_weight = load_layers(weight_ref)
    for i in range(layers):
        smooth_ref[i] = smooth_weight[i]
    store(mask_ref, mapped(lambda a: 1.0 - a.astype(jnp.float32), load_wide(active_ref)))
    store(held, operate_inner(load_wide(model_ref), smooth_weight))
    image = gathered(part_refs, held, mask_ref)
    residual = mapped(lambda a: -a, image)
    inner = operate_inner(residual, smooth_weight)
    store(residual_ref, residual)
    store(inner_ref, inner)
    lines = [dot_line(residual, residual), dot_line(residual, inner)]
    send_rows(matrix_ref, residual, lines, out_ref)


def cells_kernel(matrix_ref, *refs, count, base, begin, final):
    part_refs = refs[:count]
    got_ref, smooth_ref, mask_ref, residual_in, inner_in = refs[count : count + 5]
    refs = refs[count + 5 :]
    if not begin:
        direction_in, imaged_in, solution_in, norms_in = refs[:4]
        refs = refs[4:]
    solution_ref, residual_ref = refs[:2]
    owners = got_ref.shape[0]
    layers, tall = inner_in.shape[1:3]
    cells = layers * tall
    residual = load(residual_in)
    image = gathered(part_refs, inner_in, mask_ref)
    at = base + tall
    sums = got_ref[0, at : at + SCALARS, 0]
    for j in range(1, owners):
        sums = sums + got_ref[j, at : at + SCALARS, 0]
    at = cells + tall
    weighed = tree_sum([ref[at : at + 1] for ref in part_refs])
    line = weighed + sums[1:2]
    norm_now = full(sums[0:1])
    curvature = full(line)
    if begin:
        direction, imaged = residual, image
    else:
        ratio = norm_now / norms_in[0:1, 0:1]
        curvature = curvature + ratio * (2.0 * full(sums[2:3]) + ratio * norms_in[1:2, 0:1])
        direction = mapped(lambda r, d: r + ratio * d, residual, load(direction_in))
        imaged = mapped(lambda r, d: r + ratio * d, image, load(imaged_in))
    step_len = norm_now / curvature
    if begin:
        update = mapped(lambda d: step_len * d, direction)
    else:
        update = mapped(lambda x, d: x + step_len * d, load(solution_in), direction)
    residual = mapped(lambda r, s: r - step_len * s, residual, imaged)
    if final:
        store_wide(solution_ref, update)
        store_wide(residual_ref, residual)
        return
    store(solution_ref, update)
    store(residual_ref, residual)
    direction_ref, imaged_ref, norms_ref, inner_ref, out_ref = refs[2:]
    store(direction_ref, direction)
    store(imaged_ref, imaged)
    norms_ref[0:1] = jnp.broadcast_to(norm_now, (1, LANES))
    norms_ref[1:2] = jnp.broadcast_to(curvature, (1, LANES))
    inner = operate_inner(residual, [smooth_ref[i] for i in range(layers)])
    store(inner_ref, inner)
    lines = [dot_line(residual, residual), dot_line(residual, inner), dot_line(residual, imaged)]
    send_rows(matrix_ref, residual, lines, out_ref)


def local(sensitivity, observed, row_weight, model, smooth_weight, active):
    rows = sensitivity.shape[0]
    layers, width = smooth_weight.shape
    tall = width // LANES
    owners = lax.axis_size("mp")
    blocks = lax.axis_size("dp")
    base = rows // LANES

    weight = row_weight.reshape(base, LANES)
    target = observed.reshape(base, LANES)

    cell = jax.ShapeDtypeStruct((2, layers, tall, LANES), jnp.float32)
    field = jax.ShapeDtypeStruct(cell.shape[1:], jnp.float32)
    wide = jax.ShapeDtypeStruct(model.shape, jnp.float32)
    if tall % blocks or blocks < 4:
        raise ValueError("boundary shares")
    message = jax.ShapeDtypeStruct((owners, base + tall + SCALARS, 1, LANES), jnp.float32)
    columns = jax.ShapeDtypeStruct(((layers + 1) * tall + SUBLANES, LANES), jnp.float32)
    norms = jax.ShapeDtypeStruct((2, LANES), jnp.float32)
    vmem = pl.BlockSpec(memory_space=pltpu.VMEM)

    def call(kernel, out_shape, *operands, name, scratch=()):
        return pl.pallas_call(
            kernel,
            out_shape=out_shape,
            in_specs=[vmem] * len(operands),
            out_specs=jax.tree.map(lambda _: vmem, out_shape),
            scratch_shapes=scratch,
            compiler_params=pltpu.CompilerParams(vmem_limit_bytes=KERNEL_VMEM),
            name=name,
        )(*operands)

    def across(sent):
        return lax.all_to_all(sent, "mp", 0, 0, tiled=True)

    def along(got, subtract):
        sent = call(
            functools.partial(rows_kernel, subtract=subtract, tall=tall),
            columns,
            matrix,
            got,
            weight,
            target,
            name="rows",
        )
        return [sent] + [
            lax.ppermute(sent, "dp", [(i, i ^ s) for i in range(blocks)])
            for s in range(1, blocks)
        ]

    matrix, sent = pl.pallas_call(
        start_kernel,
        out_shape=(jax.ShapeDtypeStruct((rows, layers * width), sensitivity.dtype), message),
        in_specs=[pl.BlockSpec(memory_space=pltpu.HBM)] * 2,
        out_specs=(vmem, vmem),
        scratch_shapes=[
            pltpu.VMEM((rows // CHUNK, CHUNK) + sensitivity.shape[1:], sensitivity.dtype),
            pltpu.SemaphoreType.DMA((rows // CHUNK,)),
            pltpu.VMEM(model.shape, jnp.float32),
            pltpu.SemaphoreType.DMA,
        ],
        compiler_params=pltpu.CompilerParams(vmem_limit_bytes=KERNEL_VMEM),
        name="start",
    )(*[pltpu.with_memory_space_constraint(x, pltpu.HBM) for x in (sensitivity, model)])
    matrix = pltpu.with_memory_space_constraint(matrix, pltpu.VMEM)
    got = across(sent)
    parts = along(got, True)
    sent, residual, inner, smooth, mask = call(
        functools.partial(first_kernel, count=blocks),
        (message, cell, cell, field, cell),
        matrix,
        *parts,
        model,
        smooth_weight,
        active,
        name="first",
        scratch=[pltpu.VMEM(cell.shape, jnp.float32)],
    )
    carried = ()
    for step in range(ITERS):
        got = across(sent)
        parts = along(got, False)
        final = step == ITERS - 1
        outs = (wide, wide) if final else (cell, cell, cell, cell, norms, cell, message)
        result = call(
            functools.partial(
                cells_kernel, count=blocks, base=base, begin=step == 0, final=final
            ),
            outs,
            matrix,
            *parts,
            got,
            smooth,
            mask,
            residual,
            inner,
            *carried,
            name="cells",
        )
        if final:
            update, residual = result
        else:
            update, residual, direction, imaged, scalars, inner, sent = result
            carried = (direction, imaged, update, scalars)
    return (update, residual)


def solution(mesh):
    return jax.shard_map(
        local,
        mesh=mesh,
        in_specs=(
            P("dp", "mp", None),
            P("dp"),
            P("dp"),
            P(None, "mp", None),
            P("mp", None),
            P(None, "mp", None),
        ),
        out_specs=(P(None, "mp", None), P(None, "mp", None)),
        check_vma=False,
    )
```

```python
import functools

import jax
import jax.numpy as jnp
from jax import lax
from jax.experimental import pallas as pl
from jax.experimental.pallas import tpu as pltpu
from jax.sharding import PartitionSpec as P

GZ = 16
ITERS = 4


SMOOTHING = 0.25
COUPLING = 0.5
LANES = 128
SUBLANES = 8
SCALARS = 3
CHUNK = 64
MATRIX_BLOCKS = 2
IN_FLIGHT = 6
KERNEL_VMEM = 16 * 1024 * 1024


def tree_sum(parts):
    while len(parts) > 1:
        parts = [parts[i] + parts[i + 1] for i in range(0, len(parts), 2)]
    return parts[0]


def inner_sum(plane):
    tall = plane.shape[0]
    lane = lax.broadcasted_iota(jnp.int32, plane.shape, 1)
    line = lax.broadcasted_iota(jnp.int32, plane.shape, 0)
    position = lane % GZ
    later = jnp.where(position != GZ - 1, pltpu.roll(plane, LANES - 1, 1), 0.0)
    earlier = jnp.where(position != 0, pltpu.roll(plane, 1, 1), 0.0)
    ahead = pltpu.roll(plane, LANES - GZ, 1)
    over = jnp.where(line < tall - 1, pltpu.roll(ahead, tall - 1, 0), 0.0)
    ahead = jnp.where(lane < LANES - GZ, ahead, over)
    behind = pltpu.roll(plane, GZ, 1)
    under = jnp.where(line > 0, pltpu.roll(behind, 1, 0), 0.0)
    behind = jnp.where(lane >= GZ, behind, under)
    return later + earlier + ahead + behind


def operate_inner(field, smooth_weight):
    layers = len(field[0])
    out = [[], []]
    for f in range(2):
        for i in range(layers):
            own = field[f][i]
            beside = inner_sum(own)
            if i:
                beside = beside + field[f][i - 1]
            if i < layers - 1:
                beside = beside + field[f][i + 1]
            out[f].append(
                smooth_weight[i] * own
                + SMOOTHING * (6.0 * own - beside)
                + COUPLING * (own - field[1 - f][i])
            )
    return out


def load(ref):
    return [[ref[f, i] for i in range(ref.shape[1])] for f in range(2)]


def store(ref, field):
    for f in range(2):
        for i in range(ref.shape[1]):
            ref[f, i] = field[f][i]


def mapped(op, *fields):
    return [[op(*(x[f][i] for x in fields)) for i in range(len(fields[0][0]))] for f in range(2)]


def dot_line(one, two):
    total = None
    for f in range(2):
        for i in range(len(one[0])):
            term = one[f][i] * two[f][i]
            total = term if total is None else total + term
    return jnp.sum(total, axis=0, keepdims=True)


def full(line):
    return jnp.broadcast_to(jnp.sum(line, axis=1, keepdims=True), line.shape)


def spread(planes, count):
    return jnp.concatenate(
        [
            jnp.broadcast_to(plane[t : t + 1], (count, LANES))
            for plane in planes
            for t in range(plane.shape[0])
        ],
        axis=1,
    )


def where_block(shape, count, block, members):
    line = lax.broadcasted_iota(jnp.int32, shape, 0)
    return line // count == lax.rem(block, jnp.int32(members))


def share_of(planes, member, members):
    tall = planes[0].shape[0]
    count = tall // members
    out = jnp.zeros_like(planes[0])
    for n, plane in enumerate(planes):
        moved = pltpu.roll(plane, n * count, 0) if n else plane
        out = jnp.where(where_block(plane.shape, count, member + n, members), moved, out)
    return out


def from_shares(shares, members, n):
    tall = shares[0][1].shape[0]
    count = tall // members
    out = jnp.zeros_like(shares[0][1])
    for member, share in shares:
        out = jnp.where(where_block(share.shape, count, member + n, members), share, out)
    return pltpu.roll(out, tall - n * count, 0) if n else out


def send_rows(matrix_ref, field, lines, out_ref, ready=None):
    owners = out_ref.shape[0]
    rows = matrix_ref.shape[0]
    tall = field[0][0].shape[0]
    member = lax.axis_index("dp")
    members = lax.axis_size("dp")
    gravity_rows = member < members * 3 // 4
    chosen = [jnp.where(gravity_rows, d, s) for d, s in zip(field[0], field[1])]
    eye = lax.broadcasted_iota(jnp.int32, (LANES, LANES), 0) == lax.broadcasted_iota(
        jnp.int32, (LANES, LANES), 1
    )
    lines_in = [plane[t : t + 1] for plane in chosen for t in range(tall)]
    pieces = []
    first = 0
    if ready is None:
        first = MATRIX_BLOCKS
        vector = spread(chosen, 2 * SUBLANES).astype(jnp.bfloat16)
        product = lax.dot_general(
            vector,
            matrix_ref[0 : first * LANES],
            (((1,), (1,)), ((), ())),
            preferred_element_type=jnp.float32,
        )
    for b in range(first, rows // LANES):
        if ready is not None:
            ready(b)
        total = None
        for t, line in enumerate(lines_in):
            block = matrix_ref[b * LANES : (b + 1) * LANES, t * LANES : (t + 1) * LANES]
            term = block.astype(jnp.float32) * line
            total = term if total is None else total + term
        column = jnp.sum(total, axis=1, keepdims=True)
        pieces.append(jnp.sum(jnp.where(eye, column, 0.0), axis=0, keepdims=True))
    pieces = [product[0:1, b * LANES : (b + 1) * LANES] for b in range(first)] + pieces
    edges = [field[0][0], field[1][0], field[0][-1], field[1][-1]]
    pieces.append(share_of(edges, member, members))
    pieces += [full(line) for line in lines]
    message = jnp.concatenate(pieces, axis=0)
    for j in range(owners):
        out_ref[j, 0 : message.shape[0], 0] = message


def load_layers(ref):
    layers, width = ref.shape
    return [
        jnp.concatenate([ref[i : i + 1, t : t + LANES] for t in range(0, width, LANES)], axis=0)
        for i in range(layers)
    ]


def load_wide(ref):
    return [load_layers(ref.at[f]) for f in range(2)]


def store_wide(ref, field):
    for f in range(2):
        for i in range(ref.shape[1]):
            for t in range(ref.shape[2] // LANES):
                ref[f, i : i + 1, t * LANES : (t + 1) * LANES] = field[f][i][t : t + 1]


def start_kernel(raw_ref, far_ref, matrix_ref, out_ref, chunks, arrived, model_ref, came):
    count, height = chunks.shape[:2]

    def fetch(n):
        return pltpu.make_async_copy(
            raw_ref.at[pl.ds(n * height, height)], chunks.at[n], arrived.at[n]
        )

    model_copy = pltpu.make_async_copy(far_ref, model_ref, came)
    model_copy.start()
    for n in range(min(IN_FLIGHT, count)):
        fetch(n).start()

    def ready(b):
        for n in range(b * LANES // height, (b + 1) * LANES // height):
            fetch(n).wait()
            if n + IN_FLIGHT < count:
                fetch(n + IN_FLIGHT).start()
            block = chunks[n]
            matrix_ref[n * height : (n + 1) * height] = block.reshape(height, -1)

    model_copy.wait()
    send_rows(matrix_ref, load_wide(model_ref), [], out_ref, ready)


def rows_kernel(
    matrix_ref, got_ref, weight_ref, observed_ref, out_ref, *, subtract, tall
):
    rank = lax.axis_index("mp")
    member = lax.axis_index("dp")
    members = lax.axis_size("dp")
    owners = got_ref.shape[0]
    rows, cells = matrix_ref.shape
    blocks = rows // LANES
    values = got_ref[0, 0:blocks, 0]
    for j in range(1, owners):
        values = values + got_ref[j, 0:blocks, 0]
    if subtract:
        values = values - observed_ref[...]
    scaled = (weight_ref[...] * values).astype(jnp.bfloat16).astype(jnp.float32)
    weighed = jnp.sum(values * scaled, axis=0, keepdims=True)
    vector = spread([scaled], 2 * SUBLANES).astype(jnp.bfloat16)
    columns = jnp.dot(vector, matrix_ref[...], preferred_element_type=jnp.float32)
    pieces = [columns[0:1, t * LANES : (t + 1) * LANES] for t in range(cells // LANES)]
    count = tall // members
    shares = [got_ref[j, blocks : blocks + tall, 0] for j in range(owners)]
    held = [where_block(shares[0].shape, count, member + n, members) for n in range(4)]
    lower = held[0] | held[1]
    upper = held[2] | held[3]
    cross = None
    for j in range(owners - 1):
        term = shares[j] * pltpu.roll(shares[j + 1], 2 * count, 0)
        cross = term if cross is None else cross + term
    cross = jnp.sum(jnp.where(upper, cross, 0.0), axis=0, keepdims=True)
    weighed = weighed - 2.0 * SMOOTHING * cross
    down = jnp.maximum(rank - 1, 0)
    up = jnp.minimum(rank + 1, owners - 1)
    above = jnp.where(lower & (rank < owners - 1), got_ref[up, blocks : blocks + tall, 0], 0.0)
    below = jnp.where(upper & (rank > 0), got_ref[down, blocks : blocks + tall, 0], 0.0)
    pieces += [above + below, full(weighed), jnp.zeros((SUBLANES - 1, LANES), jnp.float32)]
    out_ref[...] = jnp.concatenate(pieces, axis=0)


def gathered(part_refs, inner_ref, mask_ref):
    layers, tall = inner_ref.shape[1:3]
    cells = layers * tall
    members = len(part_refs)
    sources = [lax.axis_index("dp") ^ s for s in range(members)]
    gravity = [q < members * 3 // 4 for q in sources]
    parts = [ref[0:cells] for ref in part_refs]
    data = [
        tree_sum([jnp.where(g, p, 0.0) for g, p in zip(gravity, parts)]),
        tree_sum([jnp.where(g, 0.0, p) for g, p in zip(gravity, parts)]),
    ]
    shares = [(q, ref[cells : cells + tall]) for q, ref in zip(sources, part_refs)]
    image = [[], []]
    for f in range(2):
        above = from_shares(shares, members, f)
        below = from_shares(shares, members, 2 + f)
        for i in range(layers):
            regular = inner_ref[f, i]
            if i == 0:
                regular = regular - SMOOTHING * below
            if i == layers - 1:
                regular = regular - SMOOTHING * above
            image[f].append(mask_ref[f, i] * (data[f][i * tall : (i + 1) * tall] + regular))
    return image


def first_kernel(matrix_ref, *refs, count):
    part_refs = refs[:count]
    model_ref, weight_ref, active_ref, out_ref, residual_ref, inner_ref = refs[count : count + 6]
    smooth_ref, mask_ref, held = refs[count + 6 :]
    layers = model_ref.shape[1]
    smooth_weight = load_layers(weight_ref)
    for i in range(layers):
        smooth_ref[i] = smooth_weight[i]
    store(mask_ref, mapped(lambda a: 1.0 - a.astype(jnp.float32), load_wide(active_ref)))
    store(held, operate_inner(load_wide(model_ref), smooth_weight))
    image = gathered(part_refs, held, mask_ref)
    residual = mapped(lambda a: -a, image)
    inner = operate_inner(residual, smooth_weight)
    store(residual_ref, residual)
    store(inner_ref, inner)
    lines = [dot_line(residual, residual), dot_line(residual, inner)]
    send_rows(matrix_ref, residual, lines, out_ref)


def cells_kernel(matrix_ref, *refs, count, base, begin, final):
    part_refs = refs[:count]
    got_ref, smooth_ref, mask_ref, residual_in, inner_in = refs[count : count + 5]
    refs = refs[count + 5 :]
    if not begin:
        direction_in, imaged_in, solution_in, norms_in = refs[:4]
        refs = refs[4:]
    solution_ref, residual_ref = refs[:2]
    owners = got_ref.shape[0]
    layers, tall = inner_in.shape[1:3]
    cells = layers * tall
    residual = load(residual_in)
    image = gathered(part_refs, inner_in, mask_ref)
    at = base + tall
    sums = got_ref[0, at : at + SCALARS, 0]
    for j in range(1, owners):
        sums = sums + got_ref[j, at : at + SCALARS, 0]
    at = cells + tall
    weighed = tree_sum([ref[at : at + 1] for ref in part_refs])
    norm_now = sums[0:1]
    curvature = weighed + sums[1:2]
    if begin:
        direction, imaged = residual, image
    else:
        ratio = norm_now / norms_in[0:1]
        curvature = curvature + ratio * (2.0 * sums[2:3] + ratio * norms_in[1:2])
        direction = mapped(lambda r, d: r + ratio * d, residual, load(direction_in))
        imaged = mapped(lambda r, d: r + ratio * d, image, load(imaged_in))
    step_len = norm_now / curvature
    if begin:
        update = mapped(lambda d: step_len * d, direction)
    else:
        update = mapped(lambda x, d: x + step_len * d, load(solution_in), direction)
    residual = mapped(lambda r, s: r - step_len * s, residual, imaged)
    if final:
        store_wide(solution_ref, update)
        store_wide(residual_ref, residual)
        return
    store(solution_ref, update)
    store(residual_ref, residual)
    direction_ref, imaged_ref, norms_ref, inner_ref, out_ref = refs[2:]
    store(direction_ref, direction)
    store(imaged_ref, imaged)
    norms_ref[0:1] = norm_now
    norms_ref[1:2] = curvature
    inner = operate_inner(residual, [smooth_ref[i] for i in range(layers)])
    store(inner_ref, inner)
    lines = [dot_line(residual, residual), dot_line(residual, inner), dot_line(residual, imaged)]
    send_rows(matrix_ref, residual, lines, out_ref)


def local(sensitivity, observed, row_weight, model, smooth_weight, active):
    rows = sensitivity.shape[0]
    layers, width = smooth_weight.shape
    tall = width // LANES
    owners = lax.axis_size("mp")
    blocks = lax.axis_size("dp")
    base = rows // LANES

    weight = row_weight.reshape(base, LANES)
    target = observed.reshape(base, LANES)

    cell = jax.ShapeDtypeStruct((2, layers, tall, LANES), jnp.float32)
    field = jax.ShapeDtypeStruct(cell.shape[1:], jnp.float32)
    wide = jax.ShapeDtypeStruct(model.shape, jnp.float32)
    if tall % blocks or blocks < 4:
        raise ValueError("boundary shares")
    message = jax.ShapeDtypeStruct((owners, base + tall + SCALARS, 1, LANES), jnp.float32)
    columns = jax.ShapeDtypeStruct(((layers + 1) * tall + SUBLANES, LANES), jnp.float32)
    norms = jax.ShapeDtypeStruct((2, LANES), jnp.float32)
    vmem = pl.BlockSpec(memory_space=pltpu.VMEM)

    def call(kernel, out_shape, *operands, name, scratch=()):
        return pl.pallas_call(
            kernel,
            out_shape=out_shape,
            in_specs=[vmem] * len(operands),
            out_specs=jax.tree.map(lambda _: vmem, out_shape),
            scratch_shapes=scratch,
            compiler_params=pltpu.CompilerParams(vmem_limit_bytes=KERNEL_VMEM),
            name=name,
        )(*operands)

    def across(sent):
        return lax.all_to_all(sent, "mp", 0, 0, tiled=True)

    def along(got, subtract):
        sent = call(
            functools.partial(rows_kernel, subtract=subtract, tall=tall),
            columns,
            matrix,
            got,
            weight,
            target,
            name="rows",
        )
        return [sent] + [
            lax.ppermute(sent, "dp", [(i, i ^ s) for i in range(blocks)])
            for s in range(1, blocks)
        ]

    matrix, sent = pl.pallas_call(
        start_kernel,
        out_shape=(jax.ShapeDtypeStruct((rows, layers * width), sensitivity.dtype), message),
        in_specs=[pl.BlockSpec(memory_space=pltpu.HBM)] * 2,
        out_specs=(vmem, vmem),
        scratch_shapes=[
            pltpu.VMEM((rows // CHUNK, CHUNK) + sensitivity.shape[1:], sensitivity.dtype),
            pltpu.SemaphoreType.DMA((rows // CHUNK,)),
            pltpu.VMEM(model.shape, jnp.float32),
            pltpu.SemaphoreType.DMA,
        ],
        compiler_params=pltpu.CompilerParams(vmem_limit_bytes=KERNEL_VMEM),
        name="start",
    )(*[pltpu.with_memory_space_constraint(x, pltpu.HBM) for x in (sensitivity, model)])
    matrix = pltpu.with_memory_space_constraint(matrix, pltpu.VMEM)
    got = across(sent)
    parts = along(got, True)
    sent, residual, inner, smooth, mask = call(
        functools.partial(first_kernel, count=blocks),
        (message, cell, cell, field, cell),
        matrix,
        *parts,
        model,
        smooth_weight,
        active,
        name="first",
        scratch=[pltpu.VMEM(cell.shape, jnp.float32)],
    )
    carried = ()
    for step in range(ITERS):
        got = across(sent)
        parts = along(got, False)
        final = step == ITERS - 1
        outs = (wide, wide) if final else (cell, cell, cell, cell, norms, cell, message)
        result = call(
            functools.partial(
                cells_kernel, count=blocks, base=base, begin=step == 0, final=final
            ),
            outs,
            matrix,
            *parts,
            got,
            smooth,
            mask,
            residual,
            inner,
            *carried,
            name="cells",
        )
        if final:
            update, residual = result
        else:
            update, residual, direction, imaged, scalars, inner, sent = result
            carried = (direction, imaged, update, scalars)
    return (update, residual)


def solution(mesh):
    return jax.shard_map(
        local,
        mesh=mesh,
        in_specs=(
            P("dp", "mp", None),
            P("dp"),
            P("dp"),
            P(None, "mp", None),
            P("mp", None),
            P(None, "mp", None),
        ),
        out_specs=(P(None, "mp", None), P(None, "mp", None)),
        check_vma=False,
    )
```
